8 devices in a mesh: b: 2 (over z, y), a: 4 (over x, core).
Axes of the slice: x: 2, y: 2, z: 1, core: 2. Of those that a mesh axis runs over, the one named last changes fastest.
Arguments:
- u: float32 [256, 256, 256], P(None, 'a', 'b')
- g: float32 [132, 256, 256], P('a', 'b')
Outputs:
- output: float32 [256, 256, 256], P(None, 'a', 'b')
All inputs are finite; a program needn't handle non-finite values.
Results may differ from the reference program's by a relative error of at most 0.001.
Values are sent between devices in bfloat16 or wider.
A program may use at most 1 GiB of HBM per device.

```python
import math
import jax
import jax.numpy as jnp
from jax import lax

N = 256
KX = 132

HI = lax.Precision.HIGHEST


def _trig(rows, cols):
    r = jnp.arange(rows, dtype=jnp.int32)[:, None]
    c = jnp.arange(cols, dtype=jnp.int32)[None, :]
    ang = ((r * c) % N).astype(jnp.float32) * (2.0 * math.pi / N)
    return jnp.cos(ang), jnp.sin(ang)


def _ksq():
    kx = jnp.arange(KX, dtype=jnp.int32)
    k = jnp.arange(N, dtype=jnp.int32)
    k = jnp.where(k <= N // 2, k, k - N)
    k2 = kx[:, None, None] ** 2 + k[None, :, None] ** 2 + k[None, None, :] ** 2
    return k2.astype(jnp.float32)


def setup_inputs(seed: int = 0) -> dict:
    k1, k2 = jax.random.split(jax.random.key(seed))
    u = jax.random.normal(k1, (N, N, N), jnp.float32)
    r = jax.random.uniform(k2, (KX, N, N), jnp.float32, -1.0, 1.0)
    g = (1.0 + 0.5 * r) / (1.0 + _ksq() / (N / 4.0) ** 2)
    g = g / jnp.sqrt(jnp.mean(g[: N // 2 + 1] ** 2))
    return {"u": u, "g": g.astype(jnp.float32)}


def _line(xr, xi, c, s, form, sign):
    f = lambda p, q: jnp.einsum(form, p.astype(jnp.float32), q.astype(jnp.float32), precision=HI)
    return f(xr, c) + sign * f(xi, s), f(xi, c) - sign * f(xr, s)


def reference(u, g):
    c, s = _trig(N, N)
    cx, sx = _trig(KX, N)
    k = jnp.arange(KX)
    keep = (k <= N // 2).astype(jnp.float32)
    wgt = jnp.where((k == 0) | (k == N // 2), 1.0, 2.0) * keep / N
    u2 = u.reshape(N, N * N)
    xr = jnp.dot(cx * keep[:, None], u2, precision=HI, preferred_element_type=jnp.float32).reshape(KX, N, N)
    xi = jnp.dot(-sx * keep[:, None], u2, precision=HI, preferred_element_type=jnp.float32).reshape(KX, N, N)
    xr, xi = _line(xr, xi, c, s, "xyz,yk->xkz", 1.0)
    xr, xi = _line(xr, xi, c, s, "xyz,zk->xyk", 1.0)
    xr, xi = xr * g, xi * g
    xr, xi = _line(xr, xi, c / N, s / N, "xyz,zk->xyk", -1.0)
    xr, xi = _line(xr, xi, c / N, s / N, "xyz,yk->xkz", -1.0)
    ar = (cx * wgt[:, None]).T
    ai = (sx * wgt[:, None]).T
    w = jnp.dot(ar, xr.reshape(KX, N * N), precision=HI, preferred_element_type=jnp.float32) - jnp.dot(ai, xi.reshape(KX, N * N), precision=HI, preferred_element_type=jnp.float32)
    return w.reshape(N, N, N)
```

```python
import functools
import math

import jax
import jax.numpy as jnp
import numpy as np
from jax import lax
from jax.experimental import pallas as pl
from jax.experimental.pallas import tpu as pltpu
from jax.sharding import PartitionSpec as P

N = 256
H = 128
KB = 33
NA = 4
NB = 2
YA = 64
CH = 3
NCH = KB // CH
F32 = jnp.float32
BF16 = jnp.bfloat16
MESH = pl.DeviceIdType.MESH


def _np_split(x):
    x = np.asarray(x, np.float32)
    out = []
    for _ in range(3):
        p = x.astype(jnp.bfloat16)
        out.append(p)
        x = x - p.astype(np.float32)
    return np.stack(out)


def _np_tables():
    r = np.arange(N)
    ang = ((r[:, None] * r[None, :]) % N).astype(np.float32) * np.float32(2.0 * math.pi / N)
    c = np.cos(ang.astype(np.float64)).astype(np.float32)
    s = np.sin(ang.astype(np.float64)).astype(np.float32)
    cs = np.stack([_np_split(c), _np_split(s)], 1)
    t1 = np.concatenate([c[:H + 1], -s[1:H]], 0)
    wgt = np.where((r == 0) | (r == H), 1.0, 2.0).astype(np.float32) / N
    t5 = np.concatenate([c[:, :H + 1] * wgt[:H + 1], -s[:, 1:H] * wgt[1:H]], 1)
    return cs, _np_split(t1), _np_split(t5)


def _split(x):
    h = x.astype(BF16)
    r = x - h.astype(F32)
    m = r.astype(BF16)
    return h, m, (r - m.astype(F32)).astype(BF16)


PAIRS = ((0, 0), (0, 1), (1, 0), (1, 1), (0, 2), (2, 0))


def _dot6(ls, rs):
    acc = None
    for i, j in PAIRS:
        d = jnp.dot(ls[i], rs[j], preferred_element_type=F32)
        acc = d if acc is None else acc + d
    return acc


def _k0(t_ref, u_ref, o_ref):
    t = jnp.swapaxes(u_ref[...], 0, 1)
    tab = [t_ref[p] for p in range(3)]
    res, ims = [], []
    for j in range(4):
        x = jnp.concatenate([t[2 * j], t[2 * j + 1]], axis=1)
        acc = _dot6(tab, _split(x))
        res += [acc[:H, :H], acc[:H, H:]]
        ims += [acc[H:, :H], acc[H:, H:]]
    re = jnp.swapaxes(jnp.stack(res), 0, 1)
    im = jnp.swapaxes(jnp.stack(ims), 0, 1)
    z = jnp.zeros((1, 8, H), F32)
    o_ref[:H, :, :H] = re
    o_ref[0:1, :, H:] = z
    o_ref[1:H, :, H:] = im[1:]
    o_ref[H:H + 1, :, :H] = im[0:1]
    o_ref[H:H + 1, :, H:] = z
    o_ref[H + 1:, :, :] = jnp.zeros((NA * KB - H - 1, 8, N), F32)


def _k2(t_ref, v_ref, o_ref):
    re = jnp.swapaxes(v_ref[:H, :, :H], 0, 1)
    im = jnp.swapaxes(jnp.concatenate([v_ref[H:H + 1, :, :H], v_ref[1:H, :, H:]], 0), 0, 1)
    tab = [t_ref[p] for p in range(3)]
    outs = []
    for j in range(4):
        x = jnp.concatenate([
            jnp.concatenate([re[2 * j], re[2 * j + 1]], axis=1),
            jnp.concatenate([im[2 * j], im[2 * j + 1]], axis=1)], axis=0)
        acc = _dot6(tab, _split(x))
        outs += [acc[:, :H], acc[:, H:]]
    o_ref[...] = jnp.swapaxes(jnp.stack(outs), 0, 1)


def _k1(cs_ref, xs_ref, g_ref, v_ref, r1, y2, r2, r3, gv, w3, w3i, t4,
        s1, q1, l1, s2, q2, s3, q3, s4, q4, l4, gsem):
    a = lax.axis_index("a")
    b = lax.axis_index("b")
    ob = 1 - b

    barrier = pltpu.get_barrier_semaphore()
    for d in range(1, NA):
        pl.semaphore_signal(barrier, inc=1, device_id=(b, lax.rem(a + d, NA)), device_id_type=MESH)
    pl.semaphore_signal(barrier, inc=1, device_id=(ob, a), device_id_type=MESH)
    pl.semaphore_wait(barrier, NA)

    def rows(blk):
        return pl.ds(pl.multiple_of(blk * YA, YA), YA)

    def planes(c):
        return pl.ds(c * CH, CH)

    own = pl.ds(pl.multiple_of(b * H, H), H)
    oth = pl.ds(pl.multiple_of(ob * H, H), H)

    def e1(c, d, to, frm):
        return pltpu.make_async_remote_copy(
            src_ref=xs_ref.at[pl.ds(to * KB + c * CH, CH)],
            dst_ref=r1.at[planes(c), rows(frm)],
            send_sem=s1.at[c, d - 1], recv_sem=q1.at[c, d - 1],
            device_id=(b, to), device_id_type=MESH)

    def e1_own(c):
        return pltpu.make_async_copy(
            xs_ref.at[pl.ds(a * KB + c * CH, CH)], r1.at[planes(c), rows(a)], l1.at[c])

    def e2(c):
        return pltpu.make_async_remote_copy(
            src_ref=y2.at[planes(c), oth], dst_ref=r2.at[planes(c)],
            send_sem=s2.at[c], recv_sem=q2.at[c], device_id=(ob, a), device_id_type=MESH)

    def e3(c):
        return pltpu.make_async_remote_copy(
            src_ref=r2.at[planes(c)], dst_ref=r3.at[planes(c)],
            send_sem=s3.at[c], recv_sem=q3.at[c], device_id=(ob, a), device_id_type=MESH)

    def e4(c, d, to, frm):
        return pltpu.make_async_remote_copy(
            src_ref=r1.at[planes(c), rows(to)],
            dst_ref=v_ref.at[pl.ds(frm * KB + c * CH, CH)],
            send_sem=s4.at[c, d - 1], recv_sem=q4.at[c, d - 1],
            device_id=(b, to), device_id_type=MESH)

    def e4_own(c):
        return pltpu.make_async_copy(
            r1.at[planes(c), rows(a)], v_ref.at[pl.ds(a * KB + c * CH, CH)], l4.at[c])

    gcopy = pltpu.make_async_copy(g_ref, gv, gsem)

    @pl.loop(0, NCH)
    def _(c):
        for d in (2, 1, 3):
            e1(c, d, lax.rem(a + d, NA), a).start()
        e1_own(c).start()

    gcopy.start()

    for p in range(3):
        for k, sl in ((0, own), (1, oth)):
            cr, sr = cs_ref[p, 0, sl, :], cs_ref[p, 1, sl, :]
            w3[p, k * N:k * N + H, :N] = cr
            w3[p, k * N:k * N + H, N:] = -sr
            w3[p, k * N + H:(k + 1) * N, :N] = sr
            w3[p, k * N + H:(k + 1) * N, N:] = cr
            cc = (cs_ref[p, 0, :, sl].astype(F32) * (1.0 / N)).astype(BF16)
            sc = (cs_ref[p, 1, :, sl].astype(F32) * (1.0 / N)).astype(BF16)
            w3i[p, :N, k * N:k * N + H] = cc
            w3i[p, :N, k * N + H:(k + 1) * N] = sc
            w3i[p, N:, k * N:k * N + H] = -sc
            w3i[p, N:, k * N + H:(k + 1) * N] = cc
            t4[p, :N, k * H:(k + 1) * H] = cc
            t4[p, N:, k * H:(k + 1) * H] = sc

    def stage2(c):
        for d in (2, 1, 3):
            frm = lax.rem(a + NA - d, NA)
            e1(c, d, frm, frm).wait_recv()
        e1_own(c).wait()

        @pl.loop(0, CH)
        def _(p):
            k = c * CH + p
            acc = _dot6([cs_ref[q].reshape(2 * N, N) for q in range(3)], _split(r1[k]))
            y2[k, :, :H] = acc[:N, :H] + acc[N:, H:]
            y2[k, :, H:] = acc[:N, H:] - acc[N:, :H]

        e2(c).start()

    def stage3(c):
        e2(c).wait_recv()

        @pl.loop(0, CH)
        def _(p):
            k = c * CH + p
            x = _split(jnp.concatenate([y2[k, own, :], r2[k]], axis=1))
            z = _dot6(x, [w3[q] for q in range(3)])
            gk = gv[k]
            z = _split(jnp.concatenate([z[:, :N] * gk, z[:, N:] * gk], axis=1))
            z = _dot6(z, [w3i[q] for q in range(3)])
            y2[k, own, :] = z[:, :N]
            r2[k] = z[:, N:]

        e3(c).start()

    def stage4(c):
        e3(c).wait_recv()

        @pl.loop(0, CH)
        def _(p):
            k = c * CH + p
            x = jnp.concatenate([y2[k, own, :], r3[k]], axis=0)
            acc = _dot6([t4[q] for q in range(3)], _split(x))
            r1[k, :, :H] = acc[:N, :H] - acc[N:, H:]
            r1[k, :, H:] = acc[:N, H:] + acc[N:, :H]

        for d in (2, 1, 3):
            e4(c, d, lax.rem(a + d, NA), a).start()
        e4_own(c).start()

    gcopy.wait()

    @pl.loop(0, NCH + 2)
    def _(i):
        @pl.when(i < NCH)
        def _():
            stage2(i)

        @pl.when(jnp.logical_and(i >= 1, i <= NCH))
        def _():
            stage3(i - 1)

        @pl.when(i >= 2)
        def _():
            stage4(i - 2)

    @pl.loop(0, NCH)
    def _(c):
        for d in range(1, NA):
            frm = lax.rem(a + NA - d, NA)
            to = lax.rem(a + d, NA)
            e1(c, d, to, a).wait_send()
            e4(c, d, to, a).wait_send()
            e4(c, d, frm, frm).wait_recv()
        e2(c).wait_send()
        e3(c).wait_send()
        e4_own(c).wait()


def solution(mesh):
    cs_np, t1_np, t5_np = _np_tables()
    dma = pltpu.SemaphoreType.DMA

    def local(u, g):
        cs, t1, t5 = jnp.asarray(cs_np), jnp.asarray(t1_np), jnp.asarray(t5_np)
        full = pl.BlockSpec((3, N, N), lambda i: (0, 0, 0))
        params = pltpu.CompilerParams(vmem_limit_bytes=60 * 2**20)
        xs = pl.pallas_call(
            _k0, grid=(YA // 8,), name="fwd_x",
            in_specs=[full, pl.BlockSpec((N, 8, H), lambda i: (0, i, 0))],
            out_specs=pl.BlockSpec((NA * KB, 8, N), lambda i: (0, i, 0)),
            out_shape=jax.ShapeDtypeStruct((NA * KB, YA, N), F32),
            compiler_params=params,
        )(t1, u)
        v = pl.pallas_call(
            _k1, name="yz",
            in_specs=[pl.BlockSpec(memory_space=pltpu.VMEM), pl.BlockSpec(memory_space=pl.ANY),
                      pl.BlockSpec(memory_space=pl.ANY)],
            out_specs=pl.BlockSpec(memory_space=pl.ANY),
            out_shape=jax.ShapeDtypeStruct((NA * KB, YA, N), F32),
            scratch_shapes=[
                pltpu.VMEM((KB, N, N), F32), pltpu.VMEM((KB, N, N), F32),
                pltpu.VMEM((KB, H, N), F32), pltpu.VMEM((KB, H, N), F32),
                pltpu.VMEM((KB, H, N), F32),
                pltpu.VMEM((3, 2 * N, 2 * N), BF16), pltpu.VMEM((3, 2 * N, 2 * N), BF16),
                pltpu.VMEM((3, 2 * N, N), BF16),
                dma((NCH, 3)), dma((NCH, 3)), dma((NCH,)),
                dma((NCH,)), dma((NCH,)), dma((NCH,)), dma((NCH,)),
                dma((NCH, 3)), dma((NCH, 3)), dma((NCH,)), dma,
            ],
            compiler_params=pltpu.CompilerParams(
                collective_id=0, has_side_effects=True, vmem_limit_bytes=60 * 2**20),
        )(cs, xs, g)
        return pl.pallas_call(
            _k2, grid=(YA // 8,), name="inv_x",
            in_specs=[full, pl.BlockSpec((NA * KB, 8, N), lambda i: (0, i, 0))],
            out_specs=pl.BlockSpec((N, 8, H), lambda i: (0, i, 0)),
            out_shape=jax.ShapeDtypeStruct((N, YA, H), F32),
            compiler_params=params,
        )(t5, v)

    return jax.shard_map(local, mesh=mesh, in_specs=(P(None, "a", "b"), P("a", "b", None)),
                         out_specs=P(None, "a", "b"), check_vma=False)
```

```python
import functools
import math

import jax
import jax.numpy as jnp
import numpy as np
from jax import lax
from jax.experimental import pallas as pl
from jax.experimental.pallas import tpu as pltpu
from jax.sharding import PartitionSpec as P

N = 256
H = 128
KB = 33
NA = 4
NB = 2
YA = 64
G = 8
NG = YA // G
US = 4
EARLY = 2
A2 = 2
A3 = 2
F32 = jnp.float32
BF16 = jnp.bfloat16
MESH = pl.DeviceIdType.MESH


def _np_split(x):
    x = np.asarray(x, np.float32)
    out = []
    for _ in range(3):
        p = x.astype(jnp.bfloat16)
        out.append(p)
        x = x - p.astype(np.float32)
    return np.stack(out)


def _np_tables():
    r = np.arange(N)
    ang = ((r[:, None] * r[None, :]) % N).astype(np.float32) * np.float32(2.0 * math.pi / N)
    c = np.cos(ang.astype(np.float64)).astype(np.float32)
    s = np.sin(ang.astype(np.float64)).astype(np.float32)
    cs = np.stack([_np_split(c), _np_split(s)], 1)
    t1 = np.concatenate([c[:H + 1], -s[1:H]], 0)
    wgt = np.where((r == 0) | (r == H), 1.0, 2.0).astype(np.float32) / N
    t5 = np.concatenate([c[:, :H + 1] * wgt[:H + 1], -s[:, 1:H] * wgt[1:H]], 1)
    return cs, _np_split(t1), _np_split(t5)


def _split(x):
    h = x.astype(BF16)
    r = x - h.astype(F32)
    m = r.astype(BF16)
    return h, m, (r - m.astype(F32)).astype(BF16)


PAIRS = ((0, 0), (0, 1), (1, 0), (1, 1), (0, 2), (2, 0))


def _dot6(ls, rs):
    acc = None
    for i, j in PAIRS:
        d = jnp.dot(ls[i], rs[j], preferred_element_type=F32)
        acc = d if acc is None else acc + d
    return acc


def _k2(t_ref, v_ref, o_ref):
    re = jnp.swapaxes(v_ref[:H, :, :H], 0, 1)
    im = jnp.swapaxes(jnp.concatenate([v_ref[H:H + 1, :, :H], v_ref[1:H, :, H:]], 0), 0, 1)
    tab = [t_ref[p] for p in range(3)]
    outs = []
    for j in range(4):
        x = jnp.concatenate([
            jnp.concatenate([re[2 * j], re[2 * j + 1]], axis=1),
            jnp.concatenate([im[2 * j], im[2 * j + 1]], axis=1)], axis=0)
        acc = _dot6(tab, _split(x))
        outs += [acc[:, :H], acc[:, H:]]
    o_ref[...] = jnp.swapaxes(jnp.stack(outs), 0, 1)


def _k1(t1_ref, cs_ref, u_ref, g_ref, v_ref, us, xs, r1, y2, r2, r3, gv, w3, w3i, t4,
        usem, gsem, s1, q1, s2, q2, s3, q3, s4, q4, l4):
    a = lax.axis_index("a")
    b = lax.axis_index("b")
    ob = 1 - b

    def ucopy(j):
        return pltpu.make_async_copy(
            u_ref.at[:, pl.ds(pl.multiple_of(j * G, G), G), :], us.at[lax.rem(j, US)],
            usem.at[lax.rem(j, US)])

    gcopy = pltpu.make_async_copy(g_ref, gv, gsem)

    @pl.loop(0, US)
    def _(j):
        ucopy(j).start()

    barrier = pltpu.get_barrier_semaphore()
    for d in range(1, NA):
        pl.semaphore_signal(barrier, inc=1, device_id=(b, lax.rem(a + d, NA)), device_id_type=MESH)
    pl.semaphore_signal(barrier, inc=1, device_id=(ob, a), device_id_type=MESH)

    def rows(blk):
        return pl.ds(pl.multiple_of(blk * YA, YA), YA)

    own = pl.ds(pl.multiple_of(b * H, H), H)
    oth = pl.ds(pl.multiple_of(ob * H, H), H)

    def e1(k, to):
        return pltpu.make_async_remote_copy(
            src_ref=xs.at[to * KB + k], dst_ref=r1.at[k, rows(a)],
            send_sem=s1, recv_sem=q1.at[k], device_id=(b, to), device_id_type=MESH)

    def e1_group(k, j, to):
        return pltpu.make_async_remote_copy(
            src_ref=xs.at[to * KB + k, pl.ds(pl.multiple_of(j * G, G), G)],
            dst_ref=r1.at[k, pl.ds(pl.multiple_of(a * YA + j * G, G), G)],
            send_sem=s1, recv_sem=q1.at[k], device_id=(b, to), device_id_type=MESH)

    def e2(k):
        return pltpu.make_async_remote_copy(
            src_ref=y2.at[k, oth], dst_ref=r2.at[k],
            send_sem=s2, recv_sem=q2.at[k], device_id=(ob, a), device_id_type=MESH)

    def e3(k):
        return pltpu.make_async_remote_copy(
            src_ref=r2.at[k], dst_ref=r3.at[k],
            send_sem=s3, recv_sem=q3.at[k], device_id=(ob, a), device_id_type=MESH)

    def e4(k, to):
        return pltpu.make_async_remote_copy(
            src_ref=r1.at[k, rows(to)], dst_ref=v_ref.at[a * KB + k],
            send_sem=s4, recv_sem=q4, device_id=(b, to), device_id_type=MESH)

    def e4_own(k):
        return pltpu.make_async_copy(r1.at[k, rows(a)], v_ref.at[a * KB + k], l4)

    def wait_bytes(ref, sem):
        pltpu.make_async_copy(ref, ref, sem).wait()

    others = [lax.rem(a + d, NA) for d in (2, 1, 3)]

    @pl.loop(0, NG)
    def _(j):
        ucopy(j).wait()
        t = jnp.swapaxes(us[lax.rem(j, US)], 0, 1)
        tab = [t1_ref[p] for p in range(3)]
        res, ims = [], []
        for q in range(G // 2):
            x = jnp.concatenate([t[2 * q], t[2 * q + 1]], axis=1)
            acc = _dot6(tab, _split(x))
            res += [acc[:H, :H], acc[:H, H:]]
            ims += [acc[H:, :H], acc[H:, H:]]
        re = jnp.swapaxes(jnp.stack(res), 0, 1)
        im = jnp.swapaxes(jnp.stack(ims), 0, 1)
        z = jnp.zeros((1, G, H), F32)
        yr = pl.ds(pl.multiple_of(j * G, G), G)
        xs[:H, yr, :H] = re
        xs[0:1, yr, H:] = z
        xs[1:H, yr, H:] = im[1:]
        xs[H:H + 1, yr, :H] = im[0:1]
        xs[H:H + 1, yr, H:] = z
        xs[H + 1:, yr, :] = jnp.zeros((NA * KB - H - 1, G, N), F32)
        r1[:, pl.ds(pl.multiple_of(a * YA + j * G, G), G), :] = xs[pl.ds(a * KB, KB), yr, :]

        @pl.when(j + US < NG)
        def _():
            ucopy(j + US).start()

        @pl.when(j == 0)
        def _():
            pl.semaphore_wait(barrier, NA)

        for k in range(EARLY):
            for to in others:
                e1_group(k, j, to).start()

    @pl.loop(EARLY, KB)
    def _(k):
        for to in others:
            e1(k, to).start()

    gcopy.start()

    def tables():
        for p in range(3):
            for k, sl in ((0, own), (1, oth)):
                cr, sr = cs_ref[p, 0, sl, :], cs_ref[p, 1, sl, :]
                w3[p, k * N:k * N + H, :N] = cr
                w3[p, k * N:k * N + H, N:] = -sr
                w3[p, k * N + H:(k + 1) * N, :N] = sr
                w3[p, k * N + H:(k + 1) * N, N:] = cr
                cc = (cs_ref[p, 0, :, sl].astype(F32) * (1.0 / N)).astype(BF16)
                sc = (cs_ref[p, 1, :, sl].astype(F32) * (1.0 / N)).astype(BF16)
                w3i[p, :N, k * N:k * N + H] = cc
                w3i[p, :N, k * N + H:(k + 1) * N] = sc
                w3i[p, N:, k * N:k * N + H] = -sc
                w3i[p, N:, k * N + H:(k + 1) * N] = cc
                t4[p, :N, k * H:(k + 1) * H] = cc
                t4[p, N:, k * H:(k + 1) * H] = sc

    def stage2(k):
        wait_bytes(r1.at[k, pl.ds(0, (NA - 1) * YA)], q1.at[k])
        acc = _dot6([cs_ref[q].reshape(2 * N, N) for q in range(3)], _split(r1[k]))
        y2[k, :, :H] = acc[:N, :H] + acc[N:, H:]
        y2[k, :, H:] = acc[:N, H:] - acc[N:, :H]
        e2(k).start()

    def stage3(k):
        e2(k).wait_recv()
        x = _split(jnp.concatenate([y2[k, own, :], r2[k]], axis=1))
        z = _dot6(x, [w3[q] for q in range(3)])
        gk = gv[k]
        z = _split(jnp.concatenate([z[:, :N] * gk, z[:, N:] * gk], axis=1))
        z = _dot6(z, [w3i[q] for q in range(3)])
        y2[k, own, :] = z[:, :N]
        r2[k] = z[:, N:]
        e3(k).start()

    def stage4(k):
        e3(k).wait_recv()
        x = jnp.concatenate([y2[k, own, :], r3[k]], axis=0)
        acc = _dot6([t4[q] for q in range(3)], _split(x))
        r1[k, :, :H] = acc[:N, :H] - acc[N:, H:]
        r1[k, :, H:] = acc[:N, H:] + acc[N:, :H]
        for to in others:
            e4(k, to).start()
        e4_own(k).start()

    @pl.loop(0, KB + A2 + A3)
    def _(i):
        @pl.when(i < KB)
        def _():
            stage2(i)

        @pl.when(i == 0)
        def _():
            tables()
            gcopy.wait()

        @pl.when(jnp.logical_and(i >= A2, i < KB + A2))
        def _():
            stage3(i - A2)

        @pl.when(i >= A2 + A3)
        def _():
            stage4(i - A2 - A3)

    blocks = xs.at[pl.ds(0, (NA - 1) * KB)]
    wait_bytes(blocks, s1)
    wait_bytes(blocks, s4)
    wait_bytes(r2, s2)
    wait_bytes(r2, s3)
    wait_bytes(xs.at[pl.ds(0, KB)], l4)
    wait_bytes(blocks, q4)


def solution(mesh):
    cs_np, t1_np, t5_np = _np_tables()
    dma = pltpu.SemaphoreType.DMA

    def local(u, g):
        cs, t1, t5 = jnp.asarray(cs_np), jnp.asarray(t1_np), jnp.asarray(t5_np)
        full = pl.BlockSpec((3, N, N), lambda i: (0, 0, 0))
        params = pltpu.CompilerParams(vmem_limit_bytes=60 * 2**20)
        any_ = pl.BlockSpec(memory_space=pl.ANY)
        vmem = pl.BlockSpec(memory_space=pltpu.VMEM)
        v = pl.pallas_call(
            _k1, name="fwd_yz",
            in_specs=[vmem, vmem, any_, any_],
            out_specs=any_,
            out_shape=jax.ShapeDtypeStruct((NA * KB, YA, N), F32),
            scratch_shapes=[
                pltpu.VMEM((US, N, G, H), F32), pltpu.VMEM((NA * KB, YA, N), F32),
                pltpu.VMEM((KB, N, N), F32), pltpu.VMEM((KB, N, N), F32),
                pltpu.VMEM((KB, H, N), F32), pltpu.VMEM((KB, H, N), F32),
                pltpu.VMEM((KB, H, N), F32),
                pltpu.VMEM((3, 2 * N, 2 * N), BF16), pltpu.VMEM((3, 2 * N, 2 * N), BF16),
                pltpu.VMEM((3, 2 * N, N), BF16),
                dma((US,)), dma, dma, dma((KB,)), dma, dma((KB,)), dma, dma((KB,)), dma, dma, dma,
            ],
            compiler_params=pltpu.CompilerParams(
                collective_id=0, has_side_effects=True, vmem_limit_bytes=60 * 2**20),
        )(t1, cs, u, g)
        return pl.pallas_call(
            _k2, grid=(YA // 8,), name="inv_x",
            in_specs=[full, pl.BlockSpec((NA * KB, 8, N), lambda i: (0, i, 0))],
            out_specs=pl.BlockSpec((N, 8, H), lambda i: (0, i, 0)),
            out_shape=jax.ShapeDtypeStruct((N, YA, H), F32),
            compiler_params=params,
        )(t5, v)

    return jax.shard_map(local, mesh=mesh, in_specs=(P(None, "a", "b"), P("a", "b", None)),
                         out_specs=P(None, "a", "b"), check_vma=False)
```

```python
import functools
import math

import jax
import jax.numpy as jnp
import numpy as np
from jax import lax
from jax.experimental import pallas as pl
from jax.experimental.pallas import tpu as pltpu
from jax.sharding import PartitionSpec as P

N = 256
H = 128
KB = 33
NA = 4
NB = 2
YA = 64
G = 8
NG = YA // G
US = 4
ALT = 2
EARLY = 2
MID = 20
LATE = 30
A2 = 2
A3 = 2
F32 = jnp.float32
BF16 = jnp.bfloat16
MESH = pl.DeviceIdType.MESH


def _np_split(x):
    x = np.asarray(x, np.float32)
    out = []
    for _ in range(3):
        p = x.astype(jnp.bfloat16)
        out.append(p)
        x = x - p.astype(np.float32)
    return np.stack(out)


def _np_tables():
    r = np.arange(N)
    ang = ((r[:, None] * r[None, :]) % N).astype(np.float32) * np.float32(2.0 * math.pi / N)
    c = np.cos(ang.astype(np.float64)).astype(np.float32)
    s = np.sin(ang.astype(np.float64)).astype(np.float32)
    cs = np.stack([_np_split(c), _np_split(s)], 1)
    t1 = np.concatenate([c[:H + 1], -s[1:H]], 0)
    wgt = np.where((r == 0) | (r == H), 1.0, 2.0).astype(np.float32) / N
    t5 = np.concatenate([c[:, :H + 1] * wgt[:H + 1], -s[:, 1:H] * wgt[1:H]], 1)
    return cs, _np_split(t1), _np_split(t5)


def _split(x):
    h = x.astype(BF16)
    r = x - h.astype(F32)
    m = r.astype(BF16)
    return h, m, (r - m.astype(F32)).astype(BF16)


PAIRS = ((0, 0), (0, 1), (1, 0), (1, 1), (0, 2), (2, 0))


def _dot6(ls, rs):
    acc = None
    for i, j in PAIRS:
        d = jnp.dot(ls[i], rs[j], preferred_element_type=F32)
        acc = d if acc is None else acc + d
    return acc


def _k2(t_ref, v_ref, o_ref):
    re = jnp.swapaxes(v_ref[:H, :, :H], 0, 1)
    im = jnp.swapaxes(jnp.concatenate([v_ref[H:H + 1, :, :H], v_ref[1:H, :, H:]], 0), 0, 1)
    tab = [t_ref[p] for p in range(3)]
    outs = []
    for j in range(4):
        x = jnp.concatenate([
            jnp.concatenate([re[2 * j], re[2 * j + 1]], axis=1),
            jnp.concatenate([im[2 * j], im[2 * j + 1]], axis=1)], axis=0)
        acc = _dot6(tab, _split(x))
        outs += [acc[:, :H], acc[:, H:]]
    o_ref[...] = jnp.swapaxes(jnp.stack(outs), 0, 1)


def _k1(t1_ref, cs_ref, u_ref, g_ref, v_ref, us, xs, r1, y2, r2, r3, gv, w3, w3i, t4,
        gp, za, zs, ya, fa, zb, vo, vx,
        usem, gsem, s1, q1, s2, q2, s3, q3, s4, q4, l4,
        gpsem, sg, qg, sa1, qa1, sa3, qa3, sa6, qa6, sa8, qa8):
    a = lax.axis_index("a")
    b = lax.axis_index("b")
    ob = 1 - b

    def ucopy(j):
        return pltpu.make_async_copy(
            u_ref.at[:, pl.ds(pl.multiple_of(j * G, G), G), :], us.at[lax.rem(j, US)],
            usem.at[lax.rem(j, US)])

    gcopy = pltpu.make_async_copy(g_ref, gv, gsem)

    @pl.loop(0, US)
    def _(j):
        ucopy(j).start()

    barrier = pltpu.get_barrier_semaphore()
    for d in range(1, NA):
        pl.semaphore_signal(barrier, inc=1, device_id=(b, lax.rem(a + d, NA)), device_id_type=MESH)
    pl.semaphore_signal(barrier, inc=1, device_id=(ob, a), device_id_type=MESH)

    def rows(blk):
        return pl.ds(pl.multiple_of(blk * YA, YA), YA)

    own = pl.ds(pl.multiple_of(b * H, H), H)
    oth = pl.ds(pl.multiple_of(ob * H, H), H)
    own_first, own_last = own, oth

    def e1(k, to):
        return pltpu.make_async_remote_copy(
            src_ref=xs.at[to * KB + k], dst_ref=r1.at[k, rows(a)],
            send_sem=s1, recv_sem=q1.at[k], device_id=(b, to), device_id_type=MESH)

    def e1_group(k, j, to):
        return pltpu.make_async_remote_copy(
            src_ref=xs.at[to * KB + k, pl.ds(pl.multiple_of(j * G, G), G)],
            dst_ref=r1.at[k, pl.ds(pl.multiple_of(a * YA + j * G, G), G)],
            send_sem=s1, recv_sem=q1.at[k], device_id=(b, to), device_id_type=MESH)

    def e2(k):
        return pltpu.make_async_remote_copy(
            src_ref=y2.at[k, oth], dst_ref=r2.at[k],
            send_sem=s2, recv_sem=q2.at[k], device_id=(ob, a), device_id_type=MESH)

    def e3(k):
        return pltpu.make_async_remote_copy(
            src_ref=r2.at[k], dst_ref=r3.at[k],
            send_sem=s3, recv_sem=q3.at[k], device_id=(ob, a), device_id_type=MESH)

    def e4(k, to):
        return pltpu.make_async_remote_copy(
            src_ref=r1.at[k, rows(to)], dst_ref=v_ref.at[a * KB + k],
            send_sem=s4, recv_sem=q4, device_id=(b, to), device_id_type=MESH)

    def e4_own(k):
        return pltpu.make_async_copy(r1.at[k, rows(a)], v_ref.at[a * KB + k], l4)

    gp_own = pltpu.make_async_copy(g_ref.at[b], gp.at[pl.ds(0, H)], gpsem)

    def gp_other():
        return pltpu.make_async_remote_copy(
            src_ref=g_ref.at[ob], dst_ref=gp.at[pl.ds(H, H)],
            send_sem=sg, recv_sem=qg, device_id=(ob, a), device_id_type=MESH)

    def a1(n, j):
        yr = pl.ds(pl.multiple_of(j * G, G), G)
        return pltpu.make_async_remote_copy(
            src_ref=xs.at[n * KB + ob, yr], dst_ref=za.at[n, yr],
            send_sem=sa1, recv_sem=qa1, device_id=(ob, a), device_id_type=MESH)

    def a3(to):
        return pltpu.make_async_remote_copy(
            src_ref=zs.at[to], dst_ref=ya.at[rows(a)],
            send_sem=sa3, recv_sem=qa3, device_id=(b, to), device_id_type=MESH)

    def a6(to):
        return pltpu.make_async_remote_copy(
            src_ref=ya.at[rows(to)], dst_ref=zb.at[a],
            send_sem=sa6, recv_sem=qa6, device_id=(b, to), device_id_type=MESH)

    def a8(n):
        return pltpu.make_async_remote_copy(
            src_ref=vx.at[n], dst_ref=v_ref.at[n * KB + b],
            send_sem=sa8, recv_sem=qa8, device_id=(ob, a), device_id_type=MESH)

    def a8_own(n):
        return pltpu.make_async_copy(vo.at[n], v_ref.at[n * KB + b], l4)

    def wait_bytes(ref, sem):
        pltpu.make_async_copy(ref, ref, sem).wait()

    others = [lax.rem(a + d, NA) for d in (2, 1, 3)]

    @pl.loop(0, NG)
    def _(j):
        ucopy(j).wait()
        t = jnp.swapaxes(us[lax.rem(j, US)], 0, 1)
        tab = [t1_ref[p] for p in range(3)]
        res, ims = [], []
        for q in range(G // 2):
            x = jnp.concatenate([t[2 * q], t[2 * q + 1]], axis=1)
            acc = _dot6(tab, _split(x))
            res += [acc[:H, :H], acc[:H, H:]]
            ims += [acc[H:, :H], acc[H:, H:]]
        re = jnp.swapaxes(jnp.stack(res), 0, 1)
        im = jnp.swapaxes(jnp.stack(ims), 0, 1)
        z = jnp.zeros((1, G, H), F32)
        yr = pl.ds(pl.multiple_of(j * G, G), G)
        xs[:H, yr, :H] = re
        xs[0:1, yr, H:] = z
        xs[1:H, yr, H:] = im[1:]
        xs[H:H + 1, yr, :H] = im[0:1]
        xs[H:H + 1, yr, H:] = z
        xs[H + 1:, yr, :] = jnp.zeros((NA * KB - H - 1, G, N), F32)
        r1[:, pl.ds(pl.multiple_of(a * YA + j * G, G), G), :] = xs[pl.ds(a * KB, KB), yr, :]

        @pl.when(j + US < NG)
        def _():
            ucopy(j + US).start()

        @pl.when(j == 0)
        def _():
            pl.semaphore_wait(barrier, NA)
            gp_other().start()

        for k in range(ALT, ALT + EARLY):
            for to in others:
                e1_group(k, j, to).start()
        for n in range(NA):
            a1(n, j).start()

    @pl.loop(ALT + EARLY, KB)
    def _(k):
        for to in others:
            e1(k, to).start()

    gcopy.start()
    gp_own.start()

    def tables():
        for p in range(3):
            for k, sl in ((0, own), (1, oth)):
                cr, sr = cs_ref[p, 0, sl, :], cs_ref[p, 1, sl, :]
                w3[p, k * N:k * N + H, :N] = cr
                w3[p, k * N:k * N + H, N:] = -sr
                w3[p, k * N + H:(k + 1) * N, :N] = sr
                w3[p, k * N + H:(k + 1) * N, N:] = cr
                cc = (cs_ref[p, 0, :, sl].astype(F32) * (1.0 / N)).astype(BF16)
                sc = (cs_ref[p, 1, :, sl].astype(F32) * (1.0 / N)).astype(BF16)
                w3i[p, :N, k * N:k * N + H] = cc
                w3i[p, :N, k * N + H:(k + 1) * N] = sc
                w3i[p, N:, k * N:k * N + H] = -sc
                w3i[p, N:, k * N + H:(k + 1) * N] = cc
                t4[p, :N, k * H:(k + 1) * H] = cc
                t4[p, N:, k * H:(k + 1) * H] = sc

    def stage2(k):
        wait_bytes(r1.at[k, pl.ds(0, (NA - 1) * YA)], q1.at[k])
        acc = _dot6([cs_ref[q].reshape(2 * N, N) for q in range(3)], _split(r1[k]))
        y2[k, :, :H] = acc[:N, :H] + acc[N:, H:]
        y2[k, :, H:] = acc[:N, H:] - acc[N:, :H]
        e2(k).start()

    def stage3(k):
        e2(k).wait_recv()
        x = _split(jnp.concatenate([y2[k, own, :], r2[k]], axis=1))
        z = _dot6(x, [w3[q] for q in range(3)])
        gk = gv[k]
        z = _split(jnp.concatenate([z[:, :N] * gk, z[:, N:] * gk], axis=1))
        z = _dot6(z, [w3i[q] for q in range(3)])
        y2[k, own, :] = z[:, :N]
        r2[k] = z[:, N:]
        e3(k).start()

    def stage4(k):
        e3(k).wait_recv()
        x = jnp.concatenate([y2[k, own, :], r3[k]], axis=0)
        acc = _dot6([t4[q] for q in range(3)], _split(x))
        r1[k, :, :H] = acc[:N, :H] - acc[N:, H:]
        r1[k, :, H:] = acc[:N, H:] + acc[N:, :H]
        for to in others:
            e4(k, to).start()
        e4_own(k).start()

    def alt_z():
        wait_bytes(za, qa1)
        x = jnp.concatenate([xs[n * KB + b] for n in range(NA)], axis=0)
        x = jnp.concatenate([x, za[...].reshape(NA * YA, N)], axis=1)
        zs[...] = _dot6(_split(x), [w3[q] for q in range(3)]).reshape(NA, YA, 2 * N)
        for to in others:
            a3(to).start()
        ya[rows(a), :] = zs[a]

    def alt_y():
        wait_bytes(zs.at[pl.ds(0, NA - 1)], qa3)
        wait_bytes(gp.at[pl.ds(H, H)], qg)
        gp_own.wait()
        for q in range(2):
            x = jnp.concatenate([ya[:, q * H:(q + 1) * H], ya[:, N + q * H:N + (q + 1) * H]], axis=1)
            acc = _dot6([cs_ref[p].reshape(2 * N, N) for p in range(3)], _split(x))
            re = acc[:N, :H] + acc[N:, H:]
            im = acc[:N, H:] - acc[N:, :H]
            fa[own_first, :H], fa[own_first, H:] = re[:H], im[:H]
            fa[own_last, :H], fa[own_last, H:] = re[H:], im[H:]
            gq = gp[:, q * H:(q + 1) * H]
            x = fa[...] * jnp.concatenate([gq, gq], axis=1)
            acc = _dot6([t4[p] for p in range(3)], _split(x))
            ya[:, q * H:(q + 1) * H] = acc[:N, :H] - acc[N:, H:]
            ya[:, N + q * H:N + (q + 1) * H] = acc[:N, H:] + acc[N:, :H]
        for to in others:
            a6(to).start()
        zb[a] = ya[rows(a), :]

    def alt_zinv():
        wait_bytes(zs.at[pl.ds(0, NA - 1)], qa6)
        z = _dot6(_split(zb[...].reshape(NA * YA, 2 * N)), [w3i[q] for q in range(3)])
        vo[...] = z[:, :N].reshape(NA, YA, N)
        vx[...] = z[:, N:].reshape(NA, YA, N)
        for n in range(NA):
            a8_own(n).start()

    @pl.loop(ALT, KB + A2 + A3)
    def _(i):
        @pl.when(i < KB)
        def _():
            stage2(i)

        @pl.when(i == ALT)
        def _():
            tables()
            gcopy.wait()
            alt_z()

        @pl.when(jnp.logical_and(i >= ALT + A2, i < KB + A2))
        def _():
            stage3(i - A2)

        @pl.when(i == MID)
        def _():
            alt_y()

        @pl.when(i == LATE)
        def _():
            alt_zinv()

        @pl.when(i == KB + A2 - 1)
        def _():
            for n in range(NA):
                a8(n).start()

        @pl.when(i >= ALT + A2 + A3)
        def _():
            stage4(i - A2 - A3)

    blocks = xs.at[pl.ds(0, (NA - 1) * (KB - ALT))]
    wait_bytes(blocks, s1)
    wait_bytes(blocks, s4)
    wait_bytes(r2.at[pl.ds(0, KB - ALT)], s2)
    wait_bytes(r2.at[pl.ds(0, KB - ALT)], s3)
    wait_bytes(gp.at[pl.ds(0, H)], sg)
    wait_bytes(za, sa1)
    wait_bytes(zs.at[pl.ds(0, NA - 1)], sa3)
    wait_bytes(zs.at[pl.ds(0, NA - 1)], sa6)
    wait_bytes(za, sa8)
    wait_bytes(xs.at[pl.ds(0, KB - ALT + NA)], l4)
    wait_bytes(blocks, q4)
    wait_bytes(za, qa8)


def solution(mesh):
    cs_np, t1_np, t5_np = _np_tables()
    dma = pltpu.SemaphoreType.DMA

    def local(u, g):
        cs, t1, t5 = jnp.asarray(cs_np), jnp.asarray(t1_np), jnp.asarray(t5_np)
        full = pl.BlockSpec((3, N, N), lambda i: (0, 0, 0))
        params = pltpu.CompilerParams(vmem_limit_bytes=60 * 2**20)
        any_ = pl.BlockSpec(memory_space=pl.ANY)
        vmem = pl.BlockSpec(memory_space=pltpu.VMEM)
        v = pl.pallas_call(
            _k1, name="fwd_yz",
            in_specs=[vmem, vmem, any_, any_],
            out_specs=any_,
            out_shape=jax.ShapeDtypeStruct((NA * KB, YA, N), F32),
            scratch_shapes=[
                pltpu.VMEM((US, N, G, H), F32), pltpu.VMEM((NA * KB, YA, N), F32),
                pltpu.VMEM((KB, N, N), F32), pltpu.VMEM((KB, N, N), F32),
                pltpu.VMEM((KB, H, N), F32), pltpu.VMEM((KB, H, N), F32),
                pltpu.VMEM((KB, H, N), F32),
                pltpu.VMEM((3, 2 * N, 2 * N), BF16), pltpu.VMEM((3, 2 * N, 2 * N), BF16),
                pltpu.VMEM((3, 2 * N, N), BF16),
                pltpu.VMEM((N, N), F32), pltpu.VMEM((NA, YA, N), F32),
                pltpu.VMEM((NA, YA, 2 * N), F32), pltpu.VMEM((N, 2 * N), F32),
                pltpu.VMEM((N, N), F32), pltpu.VMEM((NA, YA, 2 * N), F32),
                pltpu.VMEM((NA, YA, N), F32), pltpu.VMEM((NA, YA, N), F32),
                dma((US,)), dma, dma, dma((KB,)), dma, dma((KB,)), dma, dma((KB,)), dma, dma, dma,
                dma, dma, dma, dma, dma, dma, dma, dma, dma, dma, dma,
            ],
            compiler_params=pltpu.CompilerParams(
                collective_id=0, has_side_effects=True, vmem_limit_bytes=60 * 2**20),
        )(t1, cs, u, g)
        return pl.pallas_call(
            _k2, grid=(YA // 8,), name="inv_x",
            in_specs=[full, pl.BlockSpec((NA * KB, 8, N), lambda i: (0, i, 0))],
            out_specs=pl.BlockSpec((N, 8, H), lambda i: (0, i, 0)),
            out_shape=jax.ShapeDtypeStruct((N, YA, H), F32),
            compiler_params=params,
        )(t5, v)

    return jax.shard_map(local, mesh=mesh, in_specs=(P(None, "a", "b"), P("a", "b", None)),
                         out_specs=P(None, "a", "b"), check_vma=False)
```

```python
import functools
import math

import jax
import jax.numpy as jnp
import numpy as np
from jax import lax
from jax.experimental import pallas as pl
from jax.experimental.pallas import tpu as pltpu
from jax.sharding import PartitionSpec as P

N = 256
H = 128
KB = 33
NA = 4
NB = 2
YA = 64
G = 8
NG = YA // G
US = 4
ALT = 2
EARLY = 2
MID = 20
LATE = 30
NTP = 10
NM = KB - NTP
MAIN = np.arange(ALT, ALT + NM)
TAIL = np.concatenate([np.arange(ALT), np.arange(ALT + NM, KB)])
NT = NA * NTP
I5 = 31
PG = 3
A2 = 2
A3 = 2
F32 = jnp.float32
BF16 = jnp.bfloat16
MESH = pl.DeviceIdType.MESH


def _np_split(x):
    x = np.asarray(x, np.float32)
    out = []
    for _ in range(3):
        p = x.astype(jnp.bfloat16)
        out.append(p)
        x = x - p.astype(np.float32)
    return np.stack(out)


def _np_tables():
    r = np.arange(N)
    ang = ((r[:, None] * r[None, :]) % N).astype(np.float32) * np.float32(2.0 * math.pi / N)
    c = np.cos(ang.astype(np.float64)).astype(np.float32)
    s = np.sin(ang.astype(np.float64)).astype(np.float32)
    cs = np.stack([_np_split(c), _np_split(s)], 1)
    t1 = np.concatenate([c[:H + 1], -s[1:H]], 0)
    kx = np.arange(NA * KB)
    wgt = np.where((kx == 0) | (kx == H), 1.0, 2.0) * (kx <= H) / N
    kc = np.minimum(kx, N - 1)
    cr = (c[:, kc] * wgt).astype(np.float32)
    ci = (-s[:, kc] * wgt).astype(np.float32)
    blk = kx.reshape(NA, KB)
    main = blk[:, MAIN].ravel()
    tail = blk[:, TAIL].ravel()
    pad = np.zeros((N, H - main.size), np.float32)
    t5m = np.concatenate([cr[:, main], pad, ci[:, main], pad], 1)
    t5t = _np_split(np.concatenate([cr[:, tail], ci[:, tail]], 1))
    t5t = np.concatenate([t5t[i] for i, _ in PAIRS], 1)
    return cs, _np_split(t1), _np_split(t5m), t5t


def _split(x):
    h = x.astype(BF16)
    r = x - h.astype(F32)
    m = r.astype(BF16)
    return h, m, (r - m.astype(F32)).astype(BF16)


PAIRS = ((0, 0), (0, 1), (1, 0), (1, 1), (0, 2), (2, 0))


def _dot6(ls, rs):
    acc = None
    for i, j in PAIRS:
        d = jnp.dot(ls[i], rs[j], preferred_element_type=F32)
        acc = d if acc is None else acc + d
    return acc


def _k2(t_ref, w_ref, v_ref, o_ref, buf, vt, isem, vsem, osem):
    def yr(j):
        return pl.ds(pl.multiple_of(j * G, G), G)

    def rd(j):
        return pltpu.make_async_copy(w_ref.at[j], buf.at[j], isem.at[j])

    def wr(j):
        return pltpu.make_async_copy(buf.at[j], o_ref.at[:, yr(j), :], osem.at[j])

    vcopy = pltpu.make_async_copy(v_ref, vt, vsem)
    vcopy.start()

    @pl.loop(0, NG)
    def _(j):
        rd(j).start()

    vcopy.wait()

    @pl.loop(0, NG)
    def _(j):
        t = jnp.swapaxes(vt[:, yr(j), :], 0, 1)
        outs = []
        for q in range(G // 2):
            x = jnp.concatenate([
                jnp.concatenate([t[2 * q][:, :H], t[2 * q + 1][:, :H]], axis=1),
                jnp.concatenate([t[2 * q][:, H:], t[2 * q + 1][:, H:]], axis=1)], axis=0)
            p = _split(x)
            x = jnp.concatenate([p[k] for _, k in PAIRS], axis=0)
            acc = jnp.dot(t_ref[...], x, preferred_element_type=F32)
            outs += [acc[:, :H], acc[:, H:]]
        rd(j).wait()
        buf[j] += jnp.swapaxes(jnp.stack(outs), 0, 1)
        wr(j).start()

    @pl.loop(0, NG)
    def _(j):
        wr(j).wait()


def _k1(t1_ref, t5_ref, cs_ref, u_ref, g_ref, w_ref, vt_ref, us, v4, xs, r1, y2, r2, r3, gv, w3, w3i, t4,
        gp, za, zs, ya, fa, zb, vo, vx,
        usem, gsem, s1, q1, s2, q2, s3, q3, s4, q4, l4,
        gpsem, sg, qg, sa1, qa1, sa3, qa3, sa6, qa6, sa8, qa8, q4t, osem):
    a = lax.axis_index("a")
    b = lax.axis_index("b")
    ob = 1 - b

    def ucopy(j):
        return pltpu.make_async_copy(
            u_ref.at[:, pl.ds(pl.multiple_of(j * G, G), G), :], us.at[lax.rem(j, US)],
            usem.at[lax.rem(j, US)])

    gcopy = pltpu.make_async_copy(g_ref, gv, gsem)

    @pl.loop(0, US)
    def _(j):
        ucopy(j).start()

    barrier = pltpu.get_barrier_semaphore()
    for d in range(1, NA):
        pl.semaphore_signal(barrier, inc=1, device_id=(b, lax.rem(a + d, NA)), device_id_type=MESH)
    pl.semaphore_signal(barrier, inc=1, device_id=(ob, a), device_id_type=MESH)

    def rows(blk):
        return pl.ds(pl.multiple_of(blk * YA, YA), YA)

    own = pl.ds(pl.multiple_of(b * H, H), H)
    oth = pl.ds(pl.multiple_of(ob * H, H), H)
    own_first, own_last = own, oth

    def e1(k, to):
        return pltpu.make_async_remote_copy(
            src_ref=xs.at[to * KB + k], dst_ref=r1.at[k, rows(a)],
            send_sem=s1, recv_sem=q1.at[k], device_id=(b, to), device_id_type=MESH)

    def e1_group(k, j, to):
        return pltpu.make_async_remote_copy(
            src_ref=xs.at[to * KB + k, pl.ds(pl.multiple_of(j * G, G), G)],
            dst_ref=r1.at[k, pl.ds(pl.multiple_of(a * YA + j * G, G), G)],
            send_sem=s1, recv_sem=q1.at[k], device_id=(b, to), device_id_type=MESH)

    def e2(k):
        return pltpu.make_async_remote_copy(
            src_ref=y2.at[k, oth], dst_ref=r2.at[k],
            send_sem=s2, recv_sem=q2.at[k], device_id=(ob, a), device_id_type=MESH)

    def e3(k):
        return pltpu.make_async_remote_copy(
            src_ref=r2.at[k], dst_ref=r3.at[k],
            send_sem=s3, recv_sem=q3.at[k], device_id=(ob, a), device_id_type=MESH)

    def e4(k, to):
        return pltpu.make_async_remote_copy(
            src_ref=r1.at[k, rows(to)], dst_ref=v4.at[a * NM + k - ALT],
            send_sem=s4, recv_sem=q4, device_id=(b, to), device_id_type=MESH)

    def e4_tail(k, to):
        return pltpu.make_async_remote_copy(
            src_ref=r1.at[k, rows(to)], dst_ref=vt_ref.at[a * NTP + k - NM],
            send_sem=s4, recv_sem=q4t, device_id=(b, to), device_id_type=MESH)

    def e4_tail_own(k):
        return pltpu.make_async_copy(r1.at[k, rows(a)], vt_ref.at[a * NTP + k - NM], l4)

    gp_own = pltpu.make_async_copy(g_ref.at[b], gp.at[pl.ds(0, H)], gpsem)

    def gp_other():
        return pltpu.make_async_remote_copy(
            src_ref=g_ref.at[ob], dst_ref=gp.at[pl.ds(H, H)],
            send_sem=sg, recv_sem=qg, device_id=(ob, a), device_id_type=MESH)

    def a1(n, j):
        yr = pl.ds(pl.multiple_of(j * G, G), G)
        return pltpu.make_async_remote_copy(
            src_ref=xs.at[n * KB + ob, yr], dst_ref=za.at[n, yr],
            send_sem=sa1, recv_sem=qa1, device_id=(ob, a), device_id_type=MESH)

    def a3(to):
        return pltpu.make_async_remote_copy(
            src_ref=zs.at[to], dst_ref=ya.at[rows(a)],
            send_sem=sa3, recv_sem=qa3, device_id=(b, to), device_id_type=MESH)

    def a6(to):
        return pltpu.make_async_remote_copy(
            src_ref=ya.at[rows(to)], dst_ref=zb.at[a],
            send_sem=sa6, recv_sem=qa6, device_id=(b, to), device_id_type=MESH)

    def a8(n):
        return pltpu.make_async_remote_copy(
            src_ref=vx.at[n], dst_ref=vt_ref.at[n * NTP + b],
            send_sem=sa8, recv_sem=qa8, device_id=(ob, a), device_id_type=MESH)

    def a8_own(n):
        return pltpu.make_async_copy(vo.at[n], vt_ref.at[n * NTP + b], l4)

    def wait_bytes(ref, sem):
        pltpu.make_async_copy(ref, ref, sem).wait()

    others = [lax.rem(a + d, NA) for d in (2, 1, 3)]

    @pl.loop(0, NG)
    def _(j):
        ucopy(j).wait()
        t = jnp.swapaxes(us[lax.rem(j, US)], 0, 1)
        tab = [t1_ref[p] for p in range(3)]
        res, ims = [], []
        for q in range(G // 2):
            x = jnp.concatenate([t[2 * q], t[2 * q + 1]], axis=1)
            acc = _dot6(tab, _split(x))
            res += [acc[:H, :H], acc[:H, H:]]
            ims += [acc[H:, :H], acc[H:, H:]]
        re = jnp.swapaxes(jnp.stack(res), 0, 1)
        im = jnp.swapaxes(jnp.stack(ims), 0, 1)
        z = jnp.zeros((1, G, H), F32)
        yr = pl.ds(pl.multiple_of(j * G, G), G)
        xs[:H, yr, :H] = re
        xs[0:1, yr, H:] = z
        xs[1:H, yr, H:] = im[1:]
        xs[H:H + 1, yr, :H] = im[0:1]
        xs[H:H + 1, yr, H:] = z
        xs[H + 1:, yr, :] = jnp.zeros((NA * KB - H - 1, G, N), F32)
        r1[:, pl.ds(pl.multiple_of(a * YA + j * G, G), G), :] = xs[pl.ds(a * KB, KB), yr, :]

        @pl.when(j + US < NG)
        def _():
            ucopy(j + US).start()

        @pl.when(j == 0)
        def _():
            pl.semaphore_wait(barrier, NA)
            gp_other().start()

        for k in range(ALT, ALT + EARLY):
            for to in others:
                e1_group(k, j, to).start()
        for n in range(NA):
            a1(n, j).start()

    @pl.loop(ALT + EARLY, KB)
    def _(k):
        for to in others:
            e1(k, to).start()

    gcopy.start()
    gp_own.start()

    def tables():
        for p in range(3):
            for k, sl in ((0, own), (1, oth)):
                cr, sr = cs_ref[p, 0, sl, :], cs_ref[p, 1, sl, :]
                w3[p, k * N:k * N + H, :N] = cr
                w3[p, k * N:k * N + H, N:] = -sr
                w3[p, k * N + H:(k + 1) * N, :N] = sr
                w3[p, k * N + H:(k + 1) * N, N:] = cr
                cc = (cs_ref[p, 0, :, sl].astype(F32) * (1.0 / N)).astype(BF16)
                sc = (cs_ref[p, 1, :, sl].astype(F32) * (1.0 / N)).astype(BF16)
                w3i[p, :N, k * N:k * N + H] = cc
                w3i[p, :N, k * N + H:(k + 1) * N] = sc
                w3i[p, N:, k * N:k * N + H] = -sc
                w3i[p, N:, k * N + H:(k + 1) * N] = cc
                t4[p, :N, k * H:(k + 1) * H] = cc
                t4[p, N:, k * H:(k + 1) * H] = sc

    def stage2(k):
        wait_bytes(r1.at[k, pl.ds(0, (NA - 1) * YA)], q1.at[k])
        acc = _dot6([cs_ref[q].reshape(2 * N, N) for q in range(3)], _split(r1[k]))
        y2[k, :, :H] = acc[:N, :H] + acc[N:, H:]
        y2[k, :, H:] = acc[:N, H:] - acc[N:, :H]
        e2(k).start()

    def stage3(k):
        e2(k).wait_recv()
        x = _split(jnp.concatenate([y2[k, own, :], r2[k]], axis=1))
        z = _dot6(x, [w3[q] for q in range(3)])
        gk = gv[k]
        z = _split(jnp.concatenate([z[:, :N] * gk, z[:, N:] * gk], axis=1))
        z = _dot6(z, [w3i[q] for q in range(3)])
        y2[k, own, :] = z[:, :N]
        r2[k] = z[:, N:]
        e3(k).start()

    def stage4(k):
        e3(k).wait_recv()
        x = jnp.concatenate([y2[k, own, :], r3[k]], axis=0)
        acc = _dot6([t4[q] for q in range(3)], _split(x))
        r1[k, :, :H] = acc[:N, :H] - acc[N:, H:]
        r1[k, :, H:] = acc[:N, H:] + acc[N:, :H]

        @pl.when(k < ALT + NM)
        def _():
            for to in others:
                e4(k, to).start()
            v4[a * NM + k - ALT] = r1[k, rows(a), :]

        @pl.when(k >= ALT + NM)
        def _():
            for to in others:
                e4_tail(k, to).start()
            e4_tail_own(k).start()

    def alt_z():
        wait_bytes(za, qa1)
        x = jnp.concatenate([xs[n * KB + b] for n in range(NA)], axis=0)
        x = jnp.concatenate([x, za[...].reshape(NA * YA, N)], axis=1)
        zs[...] = _dot6(_split(x), [w3[q] for q in range(3)]).reshape(NA, YA, 2 * N)
        for to in others:
            a3(to).start()
        ya[rows(a), :] = zs[a]

    def alt_y():
        wait_bytes(zs.at[pl.ds(0, NA - 1)], qa3)
        wait_bytes(gp.at[pl.ds(H, H)], qg)
        gp_own.wait()
        for q in range(2):
            x = jnp.concatenate([ya[:, q * H:(q + 1) * H], ya[:, N + q * H:N + (q + 1) * H]], axis=1)
            acc = _dot6([cs_ref[p].reshape(2 * N, N) for p in range(3)], _split(x))
            re = acc[:N, :H] + acc[N:, H:]
            im = acc[:N, H:] - acc[N:, :H]
            fa[own_first, :H], fa[own_first, H:] = re[:H], im[:H]
            fa[own_last, :H], fa[own_last, H:] = re[H:], im[H:]
            gq = gp[:, q * H:(q + 1) * H]
            x = fa[...] * jnp.concatenate([gq, gq], axis=1)
            acc = _dot6([t4[p] for p in range(3)], _split(x))
            ya[:, q * H:(q + 1) * H] = acc[:N, :H] - acc[N:, H:]
            ya[:, N + q * H:N + (q + 1) * H] = acc[:N, H:] + acc[N:, :H]
        for to in others:
            a6(to).start()
        zb[a] = ya[rows(a), :]

    def alt_zinv():
        wait_bytes(zs.at[pl.ds(0, NA - 1)], qa6)
        z = _dot6(_split(zb[...].reshape(NA * YA, 2 * N)), [w3i[q] for q in range(3)])
        vo[...] = z[:, :N].reshape(NA, YA, N)
        vx[...] = z[:, N:].reshape(NA, YA, N)
        for n in range(NA):
            a8_own(n).start()

    def wr(j):
        return pltpu.make_async_copy(
            us.at[lax.rem(j, US)], w_ref.at[j], osem.at[lax.rem(j, US)])

    def inv_x(j):
        @pl.when(j >= US)
        def _():
            wr(j - US).wait()

        yr = pl.ds(pl.multiple_of(j * G, G), G)
        z = jnp.zeros((H - NA * NM, G, H), F32)
        re = jnp.swapaxes(jnp.concatenate([v4[:, yr, :H], z], axis=0), 0, 1)
        im = jnp.swapaxes(jnp.concatenate([v4[:, yr, H:], z], axis=0), 0, 1)
        tab = [t5_ref[p] for p in range(3)]
        outs = []
        for q in range(G // 2):
            x = jnp.concatenate([
                jnp.concatenate([re[2 * q], re[2 * q + 1]], axis=1),
                jnp.concatenate([im[2 * q], im[2 * q + 1]], axis=1)], axis=0)
            acc = _dot6(tab, _split(x))
            outs += [acc[:, :H], acc[:, H:]]
        us[lax.rem(j, US)] = jnp.swapaxes(jnp.stack(outs), 0, 1)
        wr(j).start()

    @pl.loop(ALT, KB + A2 + A3)
    def _(i):
        @pl.when(i < KB)
        def _():
            stage2(i)

        @pl.when(i == ALT)
        def _():
            tables()
            gcopy.wait()
            alt_z()

        @pl.when(jnp.logical_and(i >= ALT + A2, i < KB + A2))
        def _():
            stage3(i - A2)

        @pl.when(i == MID)
        def _():
            alt_y()

        @pl.when(i == LATE)
        def _():
            alt_zinv()

        @pl.when(i == KB + A2 - 1)
        def _():
            for n in range(NA):
                a8(n).start()

        @pl.when(i >= ALT + A2 + A3)
        def _():
            stage4(i - A2 - A3)

        @pl.when(i == I5)
        def _():
            wait_bytes(v4.at[pl.ds(0, (NA - 1) * NM)], q4)

        @pl.when(i >= I5)
        def _():
            @pl.loop((i - I5) * PG, jnp.minimum((i - I5 + 1) * PG, NG))
            def _(j):
                inv_x(j)

    @pl.loop(NG - US, NG)
    def _(j):
        wr(j).wait()

    blocks = xs.at[pl.ds(0, (NA - 1) * (KB - ALT))]
    wait_bytes(blocks, s1)
    wait_bytes(blocks, s4)
    wait_bytes(r2.at[pl.ds(0, KB - ALT)], s2)
    wait_bytes(r2.at[pl.ds(0, KB - ALT)], s3)
    wait_bytes(gp.at[pl.ds(0, H)], sg)
    wait_bytes(za, sa1)
    wait_bytes(zs.at[pl.ds(0, NA - 1)], sa3)
    wait_bytes(zs.at[pl.ds(0, NA - 1)], sa6)
    wait_bytes(za, sa8)
    wait_bytes(xs.at[pl.ds(0, NTP - ALT + NA)], l4)
    wait_bytes(xs.at[pl.ds(0, (NTP - ALT) * (NA - 1))], q4t)
    wait_bytes(za, qa8)


def solution(mesh):
    cs_np, t1_np, t5m_np, t5t_np = _np_tables()
    dma = pltpu.SemaphoreType.DMA

    def local(u, g):
        cs, t1, t5m, t5t = (jnp.asarray(t) for t in (cs_np, t1_np, t5m_np, t5t_np))
        any_ = pl.BlockSpec(memory_space=pl.ANY)
        vmem = pl.BlockSpec(memory_space=pltpu.VMEM)
        w, vt = pl.pallas_call(
            _k1, name="fwd_yz",
            in_specs=[vmem, vmem, vmem, any_, any_],
            out_specs=[any_, any_],
            out_shape=[jax.ShapeDtypeStruct((NG, N, G, H), F32), jax.ShapeDtypeStruct((NT, YA, N), F32)],
            scratch_shapes=[
                pltpu.VMEM((US, N, G, H), F32), pltpu.VMEM((NA * NM, YA, N), F32),
                pltpu.VMEM((NA * KB, YA, N), F32),
                pltpu.VMEM((KB, N, N), F32), pltpu.VMEM((KB, N, N), F32),
                pltpu.VMEM((KB, H, N), F32), pltpu.VMEM((KB, H, N), F32),
                pltpu.VMEM((KB, H, N), F32),
                pltpu.VMEM((3, 2 * N, 2 * N), BF16), pltpu.VMEM((3, 2 * N, 2 * N), BF16),
                pltpu.VMEM((3, 2 * N, N), BF16),
                pltpu.VMEM((N, N), F32), pltpu.VMEM((NA, YA, N), F32),
                pltpu.VMEM((NA, YA, 2 * N), F32), pltpu.VMEM((N, 2 * N), F32),
                pltpu.VMEM((N, N), F32), pltpu.VMEM((NA, YA, 2 * N), F32),
                pltpu.VMEM((NA, YA, N), F32), pltpu.VMEM((NA, YA, N), F32),
                dma((US,)), dma, dma, dma((KB,)), dma, dma((KB,)), dma, dma((KB,)), dma, dma, dma,
                dma, dma, dma, dma, dma, dma, dma, dma, dma, dma, dma, dma, dma((US,)),
            ],
            compiler_params=pltpu.CompilerParams(
                collective_id=0, has_side_effects=True, vmem_limit_bytes=63 * 2**20),
        )(t1, t5m, cs, u, g)
        return pl.pallas_call(
            _k2, name="inv_x",
            in_specs=[vmem, any_, any_], out_specs=any_,
            out_shape=jax.ShapeDtypeStruct((N, YA, H), F32),
            scratch_shapes=[
                pltpu.VMEM((NG, N, G, H), F32), pltpu.VMEM((NT, YA, N), F32),
                dma((NG,)), dma, dma((NG,))],
            compiler_params=pltpu.CompilerParams(vmem_limit_bytes=60 * 2**20),
        )(t5t, w, vt)

    return jax.shard_map(local, mesh=mesh, in_specs=(P(None, "a", "b"), P("a", "b", None)),
                         out_specs=P(None, "a", "b"), check_vma=False)
```

```python
import functools
import math

import jax
import jax.numpy as jnp
import numpy as np
from jax import lax
from jax.experimental import pallas as pl
from jax.experimental.pallas import tpu as pltpu
from jax.sharding import PartitionSpec as P

N = 256
H = 128
KB = 33
NA = 4
NB = 2
YA = 64
G = 8
NG = YA // G
VM = 52
US = 3
ALT = 2
EARLY = 2
MID = 20
LATE = 30
NTP = 10
NM = KB - NTP
MAIN = np.arange(ALT, ALT + NM)
TAIL = np.concatenate([np.arange(ALT), np.arange(ALT + NM, KB)])
NT = NA * NTP
NP = KB - ALT
GS = 6
I5 = 31
PG = 3
A2 = 2
A3 = 2
F32 = jnp.float32
BF16 = jnp.bfloat16
MESH = pl.DeviceIdType.MESH


def _np_split(x):
    x = np.asarray(x, np.float32)
    out = []
    for _ in range(3):
        p = x.astype(jnp.bfloat16)
        out.append(p)
        x = x - p.astype(np.float32)
    return np.stack(out)


def _np_tables():
    r = np.arange(N)
    ang = ((r[:, None] * r[None, :]) % N).astype(np.float32) * np.float32(2.0 * math.pi / N)
    c = np.cos(ang.astype(np.float64)).astype(np.float32)
    s = np.sin(ang.astype(np.float64)).astype(np.float32)
    cs = np.stack([_np_split(c), _np_split(s)], 1)
    t1 = np.concatenate([c[:H + 1], -s[1:H]], 0)
    kx = np.arange(NA * KB)
    wgt = np.where((kx == 0) | (kx == H), 1.0, 2.0) * (kx <= H) / N
    kc = np.minimum(kx, N - 1)
    cr = (c[:, kc] * wgt).astype(np.float32)
    ci = (-s[:, kc] * wgt).astype(np.float32)
    blk = kx.reshape(NA, KB)
    main = blk[:, MAIN].ravel()
    tail = blk[:, TAIL].ravel()
    pad = np.zeros((N, H - main.size), np.float32)
    t5m = np.concatenate([cr[:, main], pad, ci[:, main], pad], 1)
    t5t = _np_split(np.concatenate([cr[:, tail], ci[:, tail]], 1))
    t5t = np.concatenate([t5t[i] for i, _ in PAIRS], 1)
    return cs, _np_split(t1), _np_split(t5m), t5t


def _split(x):
    h = x.astype(BF16)
    r = x - h.astype(F32)
    m = r.astype(BF16)
    return h, m, (r - m.astype(F32)).astype(BF16)


PAIRS = ((0, 0), (0, 1), (1, 0), (1, 1), (0, 2), (2, 0))


def _dot6(ls, rs):
    acc = None
    for i, j in PAIRS:
        d = jnp.dot(ls[i], rs[j], preferred_element_type=F32)
        acc = d if acc is None else acc + d
    return acc


def _k2(t_ref, w_ref, v_ref, o_ref, buf, osem):
    def yr(j):
        return pl.ds(pl.multiple_of(j * G, G), G)

    def wr(j):
        return pltpu.make_async_copy(buf.at[j], o_ref.at[:, yr(j), :], osem.at[j])

    @pl.loop(0, NG)
    def _(j):
        t = jnp.swapaxes(v_ref[:, yr(j), :], 0, 1)
        outs = []
        for q in range(G // 2):
            x = jnp.concatenate([
                jnp.concatenate([t[2 * q][:, :H], t[2 * q + 1][:, :H]], axis=1),
                jnp.concatenate([t[2 * q][:, H:], t[2 * q + 1][:, H:]], axis=1)], axis=0)
            p = _split(x)
            x = jnp.concatenate([p[k] for _, k in PAIRS], axis=0)
            acc = jnp.dot(t_ref[...], x, preferred_element_type=F32)
            outs += [acc[:, :H], acc[:, H:]]
        buf[j] = w_ref[j] + jnp.swapaxes(jnp.stack(outs), 0, 1)
        wr(j).start()

    @pl.loop(0, NG)
    def _(j):
        wr(j).wait()


def _k1(t1_ref, t5_ref, cs_ref, u_ref, g_ref, w_ref, vt_ref, us, v4, xs, r1, y2, r2, r3, gv, w3, w3i, t4,
        gp, za, zs, ya, fa, zb, vx,
        usem, gsem, s1, q1, s2, q2, s3, q3, s4, q4,
        gpsem, sg, qg, sa1, qa1, sa3, qa3, sa6, qa6, sa8, qa8, q4t):
    a = lax.axis_index("a")
    b = lax.axis_index("b")
    ob = 1 - b

    def ucopy(j):
        return pltpu.make_async_copy(
            u_ref.at[:, pl.ds(pl.multiple_of(j * G, G), G), :], us.at[lax.rem(j, US)],
            usem.at[lax.rem(j, US)])

    def gcopy(k):
        return pltpu.make_async_copy(g_ref.at[k], gv.at[lax.rem(k, GS)], gsem.at[lax.rem(k, GS)])

    @pl.loop(0, US)
    def _(j):
        ucopy(j).start()

    barrier = pltpu.get_barrier_semaphore()
    for d in range(1, NA):
        pl.semaphore_signal(barrier, inc=1, device_id=(b, lax.rem(a + d, NA)), device_id_type=MESH)
    pl.semaphore_signal(barrier, inc=1, device_id=(ob, a), device_id_type=MESH)

    def rows(blk):
        return pl.ds(pl.multiple_of(blk * YA, YA), YA)

    own = pl.ds(pl.multiple_of(b * H, H), H)
    oth = pl.ds(pl.multiple_of(ob * H, H), H)
    own_first, own_last = own, oth

    def e1(k, to):
        return pltpu.make_async_remote_copy(
            src_ref=xs.at[to * KB + k], dst_ref=r1.at[k - ALT, rows(a)],
            send_sem=s1, recv_sem=q1.at[k], device_id=(b, to), device_id_type=MESH)

    def e1_group(k, j, to):
        return pltpu.make_async_remote_copy(
            src_ref=xs.at[to * KB + k, pl.ds(pl.multiple_of(j * G, G), G)],
            dst_ref=r1.at[k - ALT, pl.ds(pl.multiple_of(a * YA + j * G, G), G)],
            send_sem=s1, recv_sem=q1.at[k], device_id=(b, to), device_id_type=MESH)

    def e2(k):
        return pltpu.make_async_remote_copy(
            src_ref=y2.at[k - ALT, oth], dst_ref=r2.at[k - ALT],
            send_sem=s2, recv_sem=q2.at[k], device_id=(ob, a), device_id_type=MESH)

    def e3(k):
        return pltpu.make_async_remote_copy(
            src_ref=r2.at[k - ALT], dst_ref=r3.at[k - ALT],
            send_sem=s3, recv_sem=q3.at[k], device_id=(ob, a), device_id_type=MESH)

    def e4(k, to):
        return pltpu.make_async_remote_copy(
            src_ref=r1.at[k - ALT, rows(to)], dst_ref=v4.at[a * NM + k - ALT],
            send_sem=s4, recv_sem=q4, device_id=(b, to), device_id_type=MESH)

    def e4_tail(k, to):
        return pltpu.make_async_remote_copy(
            src_ref=r1.at[k - ALT, rows(to)], dst_ref=vt_ref.at[a * NTP + k - NM],
            send_sem=s4, recv_sem=q4t, device_id=(b, to), device_id_type=MESH)

    gp_own = pltpu.make_async_copy(g_ref.at[b], gp.at[pl.ds(0, H)], gpsem)

    def gp_other():
        return pltpu.make_async_remote_copy(
            src_ref=g_ref.at[ob], dst_ref=gp.at[pl.ds(H, H)],
            send_sem=sg, recv_sem=qg, device_id=(ob, a), device_id_type=MESH)

    def a1(n, j):
        yr = pl.ds(pl.multiple_of(j * G, G), G)
        return pltpu.make_async_remote_copy(
            src_ref=xs.at[n * KB + ob, yr], dst_ref=za.at[n, yr],
            send_sem=sa1, recv_sem=qa1, device_id=(ob, a), device_id_type=MESH)

    def a3(to):
        return pltpu.make_async_remote_copy(
            src_ref=zs.at[to], dst_ref=ya.at[rows(a)],
            send_sem=sa3, recv_sem=qa3, device_id=(b, to), device_id_type=MESH)

    def a6(to):
        return pltpu.make_async_remote_copy(
            src_ref=ya.at[rows(to)], dst_ref=zb.at[a],
            send_sem=sa6, recv_sem=qa6, device_id=(b, to), device_id_type=MESH)

    def a8(n):
        return pltpu.make_async_remote_copy(
            src_ref=vx.at[n], dst_ref=vt_ref.at[n * NTP + b],
            send_sem=sa8, recv_sem=qa8, device_id=(ob, a), device_id_type=MESH)

    def wait_bytes(ref, sem):
        pltpu.make_async_copy(ref, ref, sem).wait()

    others = [lax.rem(a + d, NA) for d in (2, 1, 3)]

    @pl.loop(0, NG)
    def _(j):
        ucopy(j).wait()
        t = jnp.swapaxes(us[lax.rem(j, US)], 0, 1)
        tab = [t1_ref[p] for p in range(3)]
        res, ims = [], []
        for q in range(G // 2):
            x = jnp.concatenate([t[2 * q], t[2 * q + 1]], axis=1)
            acc = _dot6(tab, _split(x))
            res += [acc[:H, :H], acc[:H, H:]]
            ims += [acc[H:, :H], acc[H:, H:]]
        re = jnp.swapaxes(jnp.stack(res), 0, 1)
        im = jnp.swapaxes(jnp.stack(ims), 0, 1)
        z = jnp.zeros((1, G, H), F32)
        yr = pl.ds(pl.multiple_of(j * G, G), G)
        xs[:H, yr, :H] = re
        xs[0:1, yr, H:] = z
        xs[1:H, yr, H:] = im[1:]
        xs[H:H + 1, yr, :H] = im[0:1]
        xs[H:H + 1, yr, H:] = z
        xs[H + 1:, yr, :] = jnp.zeros((NA * KB - H - 1, G, N), F32)
        r1[:, pl.ds(pl.multiple_of(a * YA + j * G, G), G), :] = xs[pl.ds(a * KB + ALT, NP), yr, :]

        @pl.when(j + US < NG)
        def _():
            ucopy(j + US).start()

        @pl.when(j == 0)
        def _():
            pl.semaphore_wait(barrier, NA)
            gp_other().start()

        for k in range(ALT, ALT + EARLY):
            for to in others:
                e1_group(k, j, to).start()
        for n in range(NA):
            a1(n, j).start()

    @pl.loop(ALT + EARLY, KB)
    def _(k):
        for to in others:
            e1(k, to).start()

    @pl.loop(ALT, ALT + GS)
    def _(k):
        gcopy(k).start()

    gp_own.start()

    def tables():
        for p in range(3):
            for k, sl in ((0, own), (1, oth)):
                cr, sr = cs_ref[p, 0, sl, :], cs_ref[p, 1, sl, :]
                w3[p, k * N:k * N + H, :N] = cr
                w3[p, k * N:k * N + H, N:] = -sr
                w3[p, k * N + H:(k + 1) * N, :N] = sr
                w3[p, k * N + H:(k + 1) * N, N:] = cr
                cc = (cs_ref[p, 0, :, sl].astype(F32) * (1.0 / N)).astype(BF16)
                sc = (cs_ref[p, 1, :, sl].astype(F32) * (1.0 / N)).astype(BF16)
                w3i[p, :N, k * N:k * N + H] = cc
                w3i[p, :N, k * N + H:(k + 1) * N] = sc
                w3i[p, N:, k * N:k * N + H] = -sc
                w3i[p, N:, k * N + H:(k + 1) * N] = cc
                t4[p, :N, k * H:(k + 1) * H] = cc
                t4[p, N:, k * H:(k + 1) * H] = sc

    def stage2(k):
        wait_bytes(r1.at[k - ALT, pl.ds(0, (NA - 1) * YA)], q1.at[k])
        acc = _dot6([cs_ref[q].reshape(2 * N, N) for q in range(3)], _split(r1[k - ALT]))
        y2[k - ALT, :, :H] = acc[:N, :H] + acc[N:, H:]
        y2[k - ALT, :, H:] = acc[:N, H:] - acc[N:, :H]
        e2(k).start()

    def stage3(k):
        e2(k).wait_recv()
        x = _split(jnp.concatenate([y2[k - ALT, own, :], r2[k - ALT]], axis=1))
        z = _dot6(x, [w3[q] for q in range(3)])
        gcopy(k).wait()
        gk = gv[lax.rem(k, GS)]
        z = _split(jnp.concatenate([z[:, :N] * gk, z[:, N:] * gk], axis=1))
        z = _dot6(z, [w3i[q] for q in range(3)])
        y2[k - ALT, own, :] = z[:, :N]
        r2[k - ALT] = z[:, N:]
        e3(k).start()

        @pl.when(k + GS < KB)
        def _():
            gcopy(k + GS).start()

    def stage4(k):
        e3(k).wait_recv()
        x = jnp.concatenate([y2[k - ALT, own, :], r3[k - ALT]], axis=0)
        acc = _dot6([t4[q] for q in range(3)], _split(x))
        r1[k - ALT, :, :H] = acc[:N, :H] - acc[N:, H:]
        r1[k - ALT, :, H:] = acc[:N, H:] + acc[N:, :H]

        @pl.when(k < ALT + NM)
        def _():
            for to in others:
                e4(k, to).start()
            v4[a * NM + k - ALT] = r1[k - ALT, rows(a), :]

        @pl.when(k >= ALT + NM)
        def _():
            for to in others:
                e4_tail(k, to).start()
            vt_ref[a * NTP + k - NM] = r1[k - ALT, rows(a), :]

    def alt_z():
        wait_bytes(za, qa1)
        x = jnp.concatenate([xs[n * KB + b] for n in range(NA)], axis=0)
        x = jnp.concatenate([x, za[...].reshape(NA * YA, N)], axis=1)
        zs[...] = _dot6(_split(x), [w3[q] for q in range(3)]).reshape(NA, YA, 2 * N)
        for to in others:
            a3(to).start()
        ya[rows(a), :] = zs[a]

    def alt_y():
        wait_bytes(zs.at[pl.ds(0, NA - 1)], qa3)
        wait_bytes(gp.at[pl.ds(H, H)], qg)
        gp_own.wait()
        for q in range(2):
            x = jnp.concatenate([ya[:, q * H:(q + 1) * H], ya[:, N + q * H:N + (q + 1) * H]], axis=1)
            acc = _dot6([cs_ref[p].reshape(2 * N, N) for p in range(3)], _split(x))
            re = acc[:N, :H] + acc[N:, H:]
            im = acc[:N, H:] - acc[N:, :H]
            fa[own_first, :H], fa[own_first, H:] = re[:H], im[:H]
            fa[own_last, :H], fa[own_last, H:] = re[H:], im[H:]
            gq = gp[:, q * H:(q + 1) * H]
            x = fa[...] * jnp.concatenate([gq, gq], axis=1)
            acc = _dot6([t4[p] for p in range(3)], _split(x))
            ya[:, q * H:(q + 1) * H] = acc[:N, :H] - acc[N:, H:]
            ya[:, N + q * H:N + (q + 1) * H] = acc[:N, H:] + acc[N:, :H]
        for to in others:
            a6(to).start()
        zb[a] = ya[rows(a), :]

    def alt_zinv():
        wait_bytes(zs.at[pl.ds(0, NA - 1)], qa6)
        z = _dot6(_split(zb[...].reshape(NA * YA, 2 * N)), [w3i[q] for q in range(3)])
        vx[...] = z[:, N:].reshape(NA, YA, N)
        for n in range(NA):
            vt_ref[n * NTP + b] = z[n * YA:(n + 1) * YA, :N]

    def inv_x(j):
        yr = pl.ds(pl.multiple_of(j * G, G), G)
        z = jnp.zeros((H - NA * NM, G, H), F32)
        re = jnp.swapaxes(jnp.concatenate([v4[:, yr, :H], z], axis=0), 0, 1)
        im = jnp.swapaxes(jnp.concatenate([v4[:, yr, H:], z], axis=0), 0, 1)
        tab = [t5_ref[p] for p in range(3)]
        outs = []
        for q in range(G // 2):
            x = jnp.concatenate([
                jnp.concatenate([re[2 * q], re[2 * q + 1]], axis=1),
                jnp.concatenate([im[2 * q], im[2 * q + 1]], axis=1)], axis=0)
            acc = _dot6(tab, _split(x))
            outs += [acc[:, :H], acc[:, H:]]
        w_ref[j] = jnp.swapaxes(jnp.stack(outs), 0, 1)

    @pl.loop(ALT, KB + A2 + A3)
    def _(i):
        @pl.when(i < KB)
        def _():
            stage2(i)

        @pl.when(i == ALT)
        def _():
            tables()
            alt_z()

        @pl.when(jnp.logical_and(i >= ALT + A2, i < KB + A2))
        def _():
            stage3(i - A2)

        @pl.when(i == MID)
        def _():
            alt_y()

        @pl.when(i == LATE)
        def _():
            alt_zinv()

        @pl.when(i == KB + A2 - 1)
        def _():
            for n in range(NA):
                a8(n).start()

        @pl.when(i >= ALT + A2 + A3)
        def _():
            stage4(i - A2 - A3)

        @pl.when(i == I5)
        def _():
            wait_bytes(v4.at[pl.ds(0, (NA - 1) * NM)], q4)

        @pl.when(i >= I5)
        def _():
            @pl.loop((i - I5) * PG, jnp.minimum((i - I5 + 1) * PG, NG))
            def _(j):
                inv_x(j)

    blocks = xs.at[pl.ds(0, (NA - 1) * (KB - ALT))]
    wait_bytes(blocks, s1)
    wait_bytes(blocks, s4)
    wait_bytes(r2, s2)
    wait_bytes(r2, s3)
    wait_bytes(gp.at[pl.ds(0, H)], sg)
    wait_bytes(za, sa1)
    wait_bytes(zs.at[pl.ds(0, NA - 1)], sa3)
    wait_bytes(zs.at[pl.ds(0, NA - 1)], sa6)
    wait_bytes(za, sa8)
    wait_bytes(xs.at[pl.ds(0, (NTP - ALT) * (NA - 1))], q4t)
    wait_bytes(za, qa8)


def solution(mesh):
    cs_np, t1_np, t5m_np, t5t_np = _np_tables()
    dma = pltpu.SemaphoreType.DMA

    def local(u, g):
        cs, t1, t5m, t5t = (jnp.asarray(t) for t in (cs_np, t1_np, t5m_np, t5t_np))
        any_ = pl.BlockSpec(memory_space=pl.ANY)
        vmem = pl.BlockSpec(memory_space=pltpu.VMEM)
        w, vt = pl.pallas_call(
            _k1, name="fwd_yz",
            in_specs=[vmem, vmem, vmem, any_, any_],
            out_specs=[vmem, vmem],
            out_shape=[pltpu.VMEM((NG, N, G, H), F32), pltpu.VMEM((NT, YA, N), F32)],
            scratch_shapes=[
                pltpu.VMEM((US, N, G, H), F32), pltpu.VMEM((NA * NM, YA, N), F32),
                pltpu.VMEM((NA * KB, YA, N), F32),
                pltpu.VMEM((NP, N, N), F32), pltpu.VMEM((NP, N, N), F32),
                pltpu.VMEM((NP, H, N), F32), pltpu.VMEM((NP, H, N), F32),
                pltpu.VMEM((GS, H, N), F32),
                pltpu.VMEM((3, 2 * N, 2 * N), BF16), pltpu.VMEM((3, 2 * N, 2 * N), BF16),
                pltpu.VMEM((3, 2 * N, N), BF16),
                pltpu.VMEM((N, N), F32), pltpu.VMEM((NA, YA, N), F32),
                pltpu.VMEM((NA, YA, 2 * N), F32), pltpu.VMEM((N, 2 * N), F32),
                pltpu.VMEM((N, N), F32), pltpu.VMEM((NA, YA, 2 * N), F32),
                pltpu.VMEM((NA, YA, N), F32),
                dma((US,)), dma((GS,)), dma, dma((KB,)), dma, dma((KB,)), dma, dma((KB,)), dma, dma,
                dma, dma, dma, dma, dma, dma, dma, dma, dma, dma, dma, dma,
            ],
            compiler_params=pltpu.CompilerParams(
                collective_id=0, has_side_effects=True, vmem_limit_bytes=VM * 2**20),
        )(t1, t5m, cs, u, g)
        return pl.pallas_call(
            _k2, name="inv_x",
            in_specs=[vmem, vmem, vmem], out_specs=any_,
            out_shape=jax.ShapeDtypeStruct((N, YA, H), F32),
            scratch_shapes=[
                pltpu.VMEM((NG, N, G, H), F32), dma((NG,))],
            compiler_params=pltpu.CompilerParams(vmem_limit_bytes=30 * 2**20),
        )(t5t, w, vt)

    return jax.shard_map(local, mesh=mesh, in_specs=(P(None, "a", "b"), P("a", "b", None)),
                         out_specs=P(None, "a", "b"), check_vma=False)
```

```python
import functools
import math

import jax
import jax.numpy as jnp
import numpy as np
from jax import lax
from jax.experimental import pallas as pl
from jax.experimental.pallas import tpu as pltpu
from jax.sharding import PartitionSpec as P

N = 256
H = 128
KB = 33
NA = 4
NB = 2
YA = 64
G = 8
NG = YA // G
VM = 52
US = 3
ALT = 2
EARLY = 2
MID = 20
LATE = 30
NTP = 10
NM = KB - NTP
MAIN = np.arange(ALT, ALT + NM)
TAIL = np.concatenate([np.arange(ALT), np.arange(ALT + NM, KB)])
NT = NA * NTP
REG = KB - 2
NP = KB - ALT
GS = 6
I5 = 31
PG = 3
A2 = 2
A3 = 2
F32 = jnp.float32
BF16 = jnp.bfloat16
MESH = pl.DeviceIdType.MESH


def _np_split(x):
    x = np.asarray(x, np.float32)
    out = []
    for _ in range(3):
        p = x.astype(jnp.bfloat16)
        out.append(p)
        x = x - p.astype(np.float32)
    return np.stack(out)


def _np_tables():
    r = np.arange(N)
    ang = ((r[:, None] * r[None, :]) % N).astype(np.float32) * np.float32(2.0 * math.pi / N)
    c = np.cos(ang.astype(np.float64)).astype(np.float32)
    s = np.sin(ang.astype(np.float64)).astype(np.float32)
    cs = np.stack([_np_split(c), _np_split(s)], 1)
    t1 = np.concatenate([c[:H + 1], -s[1:H]], 0)
    kx = np.arange(NA * KB)
    kx[3 * KB + REG - 1] = 2 * KB - 1
    kx[[2 * KB - 1, 4 * KB - 2, 4 * KB - 1]] = NA * KB
    wgt = np.where((kx == 0) | (kx == H), 1.0, 2.0) * (kx <= H) / N
    kc = np.minimum(kx, N - 1)
    cr = (c[:, kc] * wgt).astype(np.float32)
    ci = (-s[:, kc] * wgt).astype(np.float32)
    blk = np.arange(NA * KB).reshape(NA, KB)
    main = blk[:, MAIN].ravel()
    tail = blk[:, TAIL].ravel()
    pad = np.zeros((N, H - main.size), np.float32)
    t5m = np.concatenate([cr[:, main], pad, ci[:, main], pad], 1)
    t5t = _np_split(np.concatenate([cr[:, tail], ci[:, tail]], 1))
    t5t = np.concatenate([t5t[i] for i, _ in PAIRS], 1)
    return cs, _np_split(t1), _np_split(t5m), t5t


def _split(x):
    h = x.astype(BF16)
    r = x - h.astype(F32)
    m = r.astype(BF16)
    return h, m, (r - m.astype(F32)).astype(BF16)


PAIRS = ((0, 0), (0, 1), (1, 0), (1, 1), (0, 2), (2, 0))


def _dot6(ls, rs):
    acc = None
    for i, j in PAIRS:
        d = jnp.dot(ls[i], rs[j], preferred_element_type=F32)
        acc = d if acc is None else acc + d
    return acc


def _k2(t_ref, w_ref, v_ref, o_ref, buf, osem):
    def yr(j):
        return pl.ds(pl.multiple_of(j * G, G), G)

    def wr(j):
        return pltpu.make_async_copy(buf.at[j], o_ref.at[:, yr(j), :], osem.at[j])

    @pl.loop(0, NG)
    def _(j):
        t = jnp.swapaxes(v_ref[:, yr(j), :], 0, 1)
        outs = []
        for q in range(G // 2):
            x = jnp.concatenate([
                jnp.concatenate([t[2 * q][:, :H], t[2 * q + 1][:, :H]], axis=1),
                jnp.concatenate([t[2 * q][:, H:], t[2 * q + 1][:, H:]], axis=1)], axis=0)
            p = _split(x)
            x = jnp.concatenate([p[k] for _, k in PAIRS], axis=0)
            acc = jnp.dot(t_ref[...], x, preferred_element_type=F32)
            outs += [acc[:, :H], acc[:, H:]]
        buf[j] = w_ref[j] + jnp.swapaxes(jnp.stack(outs), 0, 1)
        wr(j).start()

    @pl.loop(0, NG)
    def _(j):
        wr(j).wait()


def _k1(t1_ref, t5_hbm, cs_hbm, u_ref, g_ref, w_ref, vt_ref, t5_ref, cs_ref, gx, us, v4, xs, r1, y2, r2, r3, gv, w3, w3i, t4,
        gp, za, zs, ya, fa, zb, vx,
        usem, gsem, s1, q1, s2, q2, s3, q3, s4, q4,
        gpsem, sg, qg, sa1, qa1, sa3, qa3, sa6, qa6, sa8, qa8, q4t,
        tsem, sgx, qgx):
    a = lax.axis_index("a")
    b = lax.axis_index("b")
    ob = 1 - b

    def ucopy(j):
        return pltpu.make_async_copy(
            u_ref.at[:, pl.ds(pl.multiple_of(j * G, G), G), :], us.at[lax.rem(j, US)],
            usem.at[lax.rem(j, US)])

    def gcopy(k):
        return pltpu.make_async_copy(g_ref.at[k], gv.at[lax.rem(k, GS)], gsem.at[lax.rem(k, GS)])

    nk = KB - lax.rem(a, 2) * (1 + a // 3)

    @pl.loop(0, US)
    def _(j):
        ucopy(j).start()

    cscopy = pltpu.make_async_copy(cs_hbm, cs_ref, tsem.at[0])
    t5copy = pltpu.make_async_copy(t5_hbm, t5_ref, tsem.at[1])
    cscopy.start()
    t5copy.start()
    for n in (2 * NTP - 1, 4 * NTP - 2, 4 * NTP - 1):
        vt_ref[n] = jnp.zeros((YA, N), F32)

    barrier = pltpu.get_barrier_semaphore()
    for d in range(1, NA):
        pl.semaphore_signal(barrier, inc=1, device_id=(b, lax.rem(a + d, NA)), device_id_type=MESH)
    pl.semaphore_signal(barrier, inc=1, device_id=(ob, a), device_id_type=MESH)

    def rows(blk):
        return pl.ds(pl.multiple_of(blk * YA, YA), YA)

    own = pl.ds(pl.multiple_of(b * H, H), H)
    oth = pl.ds(pl.multiple_of(ob * H, H), H)

    def cls(k):
        return jnp.maximum(k - (REG - 1), 0)

    def used(blk, k):
        return lax.rem(blk, 2) * (1 + blk // 3) < KB - k

    own_first, own_last = own, oth

    def home(blk, k):
        if isinstance(k, int) and k == REG - 1:
            return blk * KB + k - (blk // 3) * (2 * KB - 2)
        return blk * KB + k

    def e1(k, to, sem=0):
        return pltpu.make_async_remote_copy(
            src_ref=xs.at[home(to, k)],
            dst_ref=r1.at[k - ALT, rows(a)],
            send_sem=s1.at[sem], recv_sem=q1.at[k], device_id=(b, to), device_id_type=MESH)

    def e1_group(k, j, to):
        return pltpu.make_async_remote_copy(
            src_ref=xs.at[to * KB + k, pl.ds(pl.multiple_of(j * G, G), G)],
            dst_ref=r1.at[k - ALT, pl.ds(pl.multiple_of(a * YA + j * G, G), G)],
            send_sem=s1.at[0], recv_sem=q1.at[k], device_id=(b, to), device_id_type=MESH)

    def e2(k):
        return pltpu.make_async_remote_copy(
            src_ref=y2.at[k - ALT, oth], dst_ref=r2.at[k - ALT],
            send_sem=s2.at[cls(k)], recv_sem=q2.at[k], device_id=(ob, a), device_id_type=MESH)

    def e3(k):
        return pltpu.make_async_remote_copy(
            src_ref=r2.at[k - ALT], dst_ref=r3.at[k - ALT],
            send_sem=s3.at[cls(k)], recv_sem=q3.at[k], device_id=(ob, a), device_id_type=MESH)

    def e4(k, to):
        return pltpu.make_async_remote_copy(
            src_ref=r1.at[k - ALT, rows(to)], dst_ref=v4.at[a * NM + k - ALT],
            send_sem=s4.at[0], recv_sem=q4, device_id=(b, to), device_id_type=MESH)

    def e4_tail(k, n, to):
        return pltpu.make_async_remote_copy(
            src_ref=r1.at[k - ALT, rows(to)], dst_ref=vt_ref.at[a * NTP + k - NM],
            send_sem=s4.at[cls(k)], recv_sem=q4t.at[cls(k) * 3 + n], device_id=(b, to), device_id_type=MESH)

    gp_own = pltpu.make_async_copy(g_ref.at[b], gp.at[pl.ds(0, H)], gpsem)

    def gp_other():
        return pltpu.make_async_remote_copy(
            src_ref=g_ref.at[ob], dst_ref=gp.at[pl.ds(H, H)],
            send_sem=sg, recv_sem=qg, device_id=(ob, a), device_id_type=MESH)

    def a1(n, j):
        yr = pl.ds(pl.multiple_of(j * G, G), G)
        return pltpu.make_async_remote_copy(
            src_ref=xs.at[n * KB + ob, yr], dst_ref=za.at[n, yr],
            send_sem=sa1, recv_sem=qa1, device_id=(ob, a), device_id_type=MESH)

    def a3(to):
        return pltpu.make_async_remote_copy(
            src_ref=zs.at[to], dst_ref=ya.at[rows(a)],
            send_sem=sa3, recv_sem=qa3, device_id=(b, to), device_id_type=MESH)

    def a6(to):
        return pltpu.make_async_remote_copy(
            src_ref=ya.at[rows(to)], dst_ref=zb.at[a],
            send_sem=sa6, recv_sem=qa6, device_id=(b, to), device_id_type=MESH)

    def a8(n):
        return pltpu.make_async_remote_copy(
            src_ref=vx.at[n], dst_ref=vt_ref.at[n * NTP + b],
            send_sem=sa8, recv_sem=qa8, device_id=(ob, a), device_id_type=MESH)

    def wait_bytes(ref, sem):
        pltpu.make_async_copy(ref, ref, sem).wait()

    others = [lax.rem(a + d, NA) for d in (2, 1, 3)]
    senders = [lax.rem(a + NA - d, NA) for d in (2, 1, 3)]

    gxcopy = pltpu.make_async_remote_copy(
        src_ref=g_ref.at[KB - 1], dst_ref=gx, send_sem=sgx, recv_sem=qgx,
        device_id=(b, 3), device_id_type=MESH)

    @pl.loop(0, NG)
    def _(j):
        ucopy(j).wait()
        t = jnp.swapaxes(us[lax.rem(j, US)], 0, 1)
        tab = [t1_ref[p] for p in range(3)]
        res, ims = [], []
        for q in range(G // 2):
            x = jnp.concatenate([t[2 * q], t[2 * q + 1]], axis=1)
            acc = _dot6(tab, _split(x))
            res += [acc[:H, :H], acc[:H, H:]]
            ims += [acc[H:, :H], acc[H:, H:]]
        re = jnp.swapaxes(jnp.stack(res), 0, 1)
        im = jnp.swapaxes(jnp.stack(ims), 0, 1)
        z = jnp.zeros((1, G, H), F32)
        yr = pl.ds(pl.multiple_of(j * G, G), G)
        xs[:H, yr, :H] = re
        xs[0:1, yr, H:] = z
        xs[1:H, yr, H:] = im[1:]
        xs[H:H + 1, yr, :H] = im[0:1]
        xs[H:H + 1, yr, H:] = z
        xs[H + 1:, yr, :] = jnp.zeros((NA * KB - H - 1, G, N), F32)
        r1[:, pl.ds(pl.multiple_of(a * YA + j * G, G), G), :] = xs[pl.ds(a * KB + ALT, NP), yr, :]
        r1[REG - 1 - ALT, pl.ds(pl.multiple_of(a * YA + j * G, G), G), :] = xs[home(a, REG - 1), yr, :]

        @pl.when(j + US < NG)
        def _():
            ucopy(j + US).start()

        @pl.when(j == 0)
        def _():
            pl.semaphore_wait(barrier, NA)
            gp_other().start()

            @pl.when(a == 1)
            def _():
                gxcopy.start()

        for k in range(ALT, ALT + EARLY):
            for to in others:
                e1_group(k, j, to).start()
        for n in range(NA):
            a1(n, j).start()

    @pl.loop(ALT + EARLY, REG - 1)
    def _(k):
        for to in others:
            e1(k, to).start()

    for to in others:
        e1(REG - 1, to).start()
    for k in (REG, REG + 1):
        for n, to in enumerate(others):
            @pl.when(used(to, k))
            def _():
                e1(k, to, 1 + (k - REG) * 3 + n).start()

    cscopy.wait()

    @pl.loop(ALT, ALT + GS)
    def _(k):
        gcopy(k).start()

    gp_own.start()

    def tables():
        for p in range(3):
            for k, sl in ((0, own), (1, oth)):
                cr, sr = cs_ref[p, 0, sl, :], cs_ref[p, 1, sl, :]
                w3[p, k * N:k * N + H, :N] = cr
                w3[p, k * N:k * N + H, N:] = -sr
                w3[p, k * N + H:(k + 1) * N, :N] = sr
                w3[p, k * N + H:(k + 1) * N, N:] = cr
                cc = (cs_ref[p, 0, :, sl].astype(F32) * (1.0 / N)).astype(BF16)
                sc = (cs_ref[p, 1, :, sl].astype(F32) * (1.0 / N)).astype(BF16)
                w3i[p, :N, k * N:k * N + H] = cc
                w3i[p, :N, k * N + H:(k + 1) * N] = sc
                w3i[p, N:, k * N:k * N + H] = -sc
                w3i[p, N:, k * N + H:(k + 1) * N] = cc
                t4[p, :N, k * H:(k + 1) * H] = cc
                t4[p, N:, k * H:(k + 1) * H] = sc

    def stage2(k):
        wait_bytes(r1.at[k - ALT, pl.ds(0, (NA - 1) * YA)], q1.at[k])
        acc = _dot6([cs_ref[q].reshape(2 * N, N) for q in range(3)], _split(r1[k - ALT]))
        y2[k - ALT, :, :H] = acc[:N, :H] + acc[N:, H:]
        y2[k - ALT, :, H:] = acc[:N, H:] - acc[N:, :H]
        e2(k).start()

    def stage3(k):
        e2(k).wait_recv()
        x = _split(jnp.concatenate([y2[k - ALT, own, :], r2[k - ALT]], axis=1))
        z = _dot6(x, [w3[q] for q in range(3)])
        gcopy(k).wait()

        @pl.when(jnp.logical_and(k == REG - 1, a == 3))
        def _():
            gxcopy.wait_recv()
            gv[(REG - 1) % GS] = gx[...]

        gk = gv[lax.rem(k, GS)]
        z = _split(jnp.concatenate([z[:, :N] * gk, z[:, N:] * gk], axis=1))
        z = _dot6(z, [w3i[q] for q in range(3)])
        y2[k - ALT, own, :] = z[:, :N]
        r2[k - ALT] = z[:, N:]
        e3(k).start()

        @pl.when(k + GS < nk)
        def _():
            gcopy(k + GS).start()

    def stage4(k):
        e3(k).wait_recv()
        x = jnp.concatenate([y2[k - ALT, own, :], r3[k - ALT]], axis=0)
        acc = _dot6([t4[q] for q in range(3)], _split(x))
        r1[k - ALT, :, :H] = acc[:N, :H] - acc[N:, H:]
        r1[k - ALT, :, H:] = acc[:N, H:] + acc[N:, :H]

        @pl.when(k < ALT + NM)
        def _():
            for to in others:
                e4(k, to).start()
            v4[a * NM + k - ALT] = r1[k - ALT, rows(a), :]

        @pl.when(k >= ALT + NM)
        def _():
            for n, to in enumerate(others):
                e4_tail(k, n, to).start()
            vt_ref[a * NTP + k - NM] = r1[k - ALT, rows(a), :]

    def alt_z():
        wait_bytes(za, qa1)
        x = jnp.concatenate([xs[n * KB + b] for n in range(NA)], axis=0)
        x = jnp.concatenate([x, za[...].reshape(NA * YA, N)], axis=1)
        zs[...] = _dot6(_split(x), [w3[q] for q in range(3)]).reshape(NA, YA, 2 * N)
        for to in others:
            a3(to).start()
        ya[rows(a), :] = zs[a]

    def alt_y():
        wait_bytes(zs.at[pl.ds(0, NA - 1)], qa3)
        wait_bytes(gp.at[pl.ds(H, H)], qg)
        gp_own.wait()
        for q in range(2):
            x = jnp.concatenate([ya[:, q * H:(q + 1) * H], ya[:, N + q * H:N + (q + 1) * H]], axis=1)
            acc = _dot6([cs_ref[p].reshape(2 * N, N) for p in range(3)], _split(x))
            re = acc[:N, :H] + acc[N:, H:]
            im = acc[:N, H:] - acc[N:, :H]
            fa[own_first, :H], fa[own_first, H:] = re[:H], im[:H]
            fa[own_last, :H], fa[own_last, H:] = re[H:], im[H:]
            gq = gp[:, q * H:(q + 1) * H]
            x = fa[...] * jnp.concatenate([gq, gq], axis=1)
            acc = _dot6([t4[p] for p in range(3)], _split(x))
            ya[:, q * H:(q + 1) * H] = acc[:N, :H] - acc[N:, H:]
            ya[:, N + q * H:N + (q + 1) * H] = acc[:N, H:] + acc[N:, :H]
        for to in others:
            a6(to).start()
        zb[a] = ya[rows(a), :]

    def alt_zinv():
        wait_bytes(zs.at[pl.ds(0, NA - 1)], qa6)
        z = _dot6(_split(zb[...].reshape(NA * YA, 2 * N)), [w3i[q] for q in range(3)])
        vx[...] = z[:, N:].reshape(NA, YA, N)
        for n in range(NA):
            vt_ref[n * NTP + b] = z[n * YA:(n + 1) * YA, :N]

    def inv_x(j):
        yr = pl.ds(pl.multiple_of(j * G, G), G)
        z = jnp.zeros((H - NA * NM, G, H), F32)
        re = jnp.swapaxes(jnp.concatenate([v4[:, yr, :H], z], axis=0), 0, 1)
        im = jnp.swapaxes(jnp.concatenate([v4[:, yr, H:], z], axis=0), 0, 1)
        tab = [t5_ref[p] for p in range(3)]
        outs = []
        for q in range(G // 2):
            x = jnp.concatenate([
                jnp.concatenate([re[2 * q], re[2 * q + 1]], axis=1),
                jnp.concatenate([im[2 * q], im[2 * q + 1]], axis=1)], axis=0)
            acc = _dot6(tab, _split(x))
            outs += [acc[:, :H], acc[:, H:]]
        w_ref[j] = jnp.swapaxes(jnp.stack(outs), 0, 1)

    @pl.loop(ALT, KB + A2 + A3)
    def _(i):
        @pl.when(i < nk)
        def _():
            stage2(i)

        @pl.when(i == ALT)
        def _():
            tables()
            alt_z()

        @pl.when(jnp.logical_and(i >= ALT + A2, i < nk + A2))
        def _():
            stage3(i - A2)

        @pl.when(i == MID)
        def _():
            alt_y()

        @pl.when(i == LATE)
        def _():
            alt_zinv()

        @pl.when(i == KB + A2 - 1)
        def _():
            for n in range(NA):
                a8(n).start()

        @pl.when(jnp.logical_and(i >= ALT + A2 + A3, i < nk + A2 + A3))
        def _():
            stage4(i - A2 - A3)

        @pl.when(i == I5)
        def _():
            wait_bytes(v4.at[pl.ds(0, (NA - 1) * NM)], q4)
            t5copy.wait()

        @pl.when(i >= I5)
        def _():
            @pl.loop((i - I5) * PG, jnp.minimum((i - I5 + 1) * PG, NG))
            def _(j):
                inv_x(j)

    def blocks(n):
        return xs.at[pl.ds(0, n)]

    nr = REG - ALT
    wait_bytes(blocks((NA - 1) * nr), s1.at[0])
    wait_bytes(blocks((NA - 1) * nr), s4.at[0])
    wait_bytes(r2.at[pl.ds(0, nr)], s2.at[0])
    wait_bytes(r2.at[pl.ds(0, nr)], s3.at[0])
    for k in (REG, REG + 1):
        c = k - REG + 1

        @pl.when(used(a, k))
        def _():
            wait_bytes(blocks(NA - 1), s4.at[c])
            wait_bytes(r2.at[0], s2.at[c])
            wait_bytes(r2.at[0], s3.at[c])

        for n in range(NA - 1):
            @pl.when(used(others[n], k))
            def _():
                wait_bytes(xs.at[0], s1.at[1 + (k - REG) * 3 + n])

            @pl.when(used(senders[n], k))
            def _():
                wait_bytes(xs.at[0], q4t.at[c * 3 + n])

    @pl.when(a == 1)
    def _():
        gxcopy.wait_send()

    for n in range(NA - 1):
        wait_bytes(blocks(REG - ALT - NM), q4t.at[n])
    wait_bytes(gp.at[pl.ds(0, H)], sg)
    wait_bytes(za, sa1)
    wait_bytes(zs.at[pl.ds(0, NA - 1)], sa3)
    wait_bytes(zs.at[pl.ds(0, NA - 1)], sa6)
    wait_bytes(za, sa8)
    wait_bytes(za, qa8)


def solution(mesh):
    cs_np, t1_np, t5m_np, t5t_np = _np_tables()
    dma = pltpu.SemaphoreType.DMA

    def local(u, g):
        cs, t1, t5m, t5t = (jnp.asarray(t) for t in (cs_np, t1_np, t5m_np, t5t_np))
        any_ = pl.BlockSpec(memory_space=pl.ANY)
        vmem = pl.BlockSpec(memory_space=pltpu.VMEM)
        w, vt = pl.pallas_call(
            _k1, name="fwd_yz",
            in_specs=[vmem, any_, any_, any_, any_],
            out_specs=[vmem, vmem],
            out_shape=[pltpu.VMEM((NG, N, G, H), F32), pltpu.VMEM((NT, YA, N), F32)],
            scratch_shapes=[
                pltpu.VMEM((3, N, N), BF16), pltpu.VMEM((3, 2, N, N), BF16), pltpu.VMEM((H, N), F32),
                pltpu.VMEM((US, N, G, H), F32), pltpu.VMEM((NA * NM, YA, N), F32),
                pltpu.VMEM((NA * KB, YA, N), F32),
                pltpu.VMEM((NP, N, N), F32), pltpu.VMEM((NP, N, N), F32),
                pltpu.VMEM((NP, H, N), F32), pltpu.VMEM((NP, H, N), F32),
                pltpu.VMEM((GS, H, N), F32),
                pltpu.VMEM((3, 2 * N, 2 * N), BF16), pltpu.VMEM((3, 2 * N, 2 * N), BF16),
                pltpu.VMEM((3, 2 * N, N), BF16),
                pltpu.VMEM((N, N), F32), pltpu.VMEM((NA, YA, N), F32),
                pltpu.VMEM((NA, YA, 2 * N), F32), pltpu.VMEM((N, 2 * N), F32),
                pltpu.VMEM((N, N), F32), pltpu.VMEM((NA, YA, 2 * N), F32),
                pltpu.VMEM((NA, YA, N), F32),
                dma((US,)), dma((GS,)), dma((7,)), dma((KB,)), dma((3,)), dma((KB,)), dma((3,)), dma((KB,)),
                dma((3,)), dma,
                dma, dma, dma, dma, dma, dma, dma, dma, dma, dma, dma, dma((9,)),
                dma((2,)), dma, dma,
            ],
            compiler_params=pltpu.CompilerParams(
                collective_id=0, has_side_effects=True, vmem_limit_bytes=VM * 2**20),
        )(t1, t5m, cs, u, g)
        return pl.pallas_call(
            _k2, name="inv_x",
            in_specs=[vmem, vmem, vmem], out_specs=any_,
            out_shape=jax.ShapeDtypeStruct((N, YA, H), F32),
            scratch_shapes=[
                pltpu.VMEM((NG, N, G, H), F32), dma((NG,))],
            compiler_params=pltpu.CompilerParams(vmem_limit_bytes=30 * 2**20),
        )(t5t, w, vt)

    return jax.shard_map(local, mesh=mesh, in_specs=(P(None, "a", "b"), P("a", "b", None)),
                         out_specs=P(None, "a", "b"), check_vma=False)
```

```python
import functools
import math

import jax
import jax.numpy as jnp
import numpy as np
from jax import lax
from jax.experimental import pallas as pl
from jax.experimental.pallas import tpu as pltpu
from jax.sharding import PartitionSpec as P

N = 256
H = 128
KB = 33
NA = 4
NB = 2
YA = 64
G = 8
NG = YA // G
VM = 52
US = 3
ALT = 2
EARLY = 2
MID = 20
LATE = 30
NTP = 10
NM = KB - NTP
MAIN = np.arange(ALT, ALT + NM)
MIDS = (2, 3, 4, 5, 6)
ENDS = (0, 1, 7, 8, 9)
TAIL = np.concatenate([np.arange(ALT), np.arange(ALT + NM, KB)])
NT = NA * NTP
REG = KB - 2
NP = KB - ALT
QS = 8
GS = 6
I5 = 31
PG = 3
A2 = 2
A3 = 2
F32 = jnp.float32
BF16 = jnp.bfloat16
MESH = pl.DeviceIdType.MESH


def _np_split(x):
    x = np.asarray(x, np.float32)
    out = []
    for _ in range(3):
        p = x.astype(jnp.bfloat16)
        out.append(p)
        x = x - p.astype(np.float32)
    return np.stack(out)


def _np_tables():
    r = np.arange(N)
    ang = ((r[:, None] * r[None, :]) % N).astype(np.float32) * np.float32(2.0 * math.pi / N)
    c = np.cos(ang.astype(np.float64)).astype(np.float32)
    s = np.sin(ang.astype(np.float64)).astype(np.float32)
    cs = np.stack([_np_split(c), _np_split(s)], 1)
    t1 = np.concatenate([c[:H + 1], -s[1:H]], 0)
    kx = np.arange(NA * KB)
    kx[3 * KB + REG - 1] = 2 * KB - 1
    kx[[2 * KB - 1, 4 * KB - 2, 4 * KB - 1]] = NA * KB
    wgt = np.where((kx == 0) | (kx == H), 1.0, 2.0) * (kx <= H) / N
    kc = np.minimum(kx, N - 1)
    cr = (c[:, kc] * wgt).astype(np.float32)
    ci = (-s[:, kc] * wgt).astype(np.float32)
    blk = np.arange(NA * KB).reshape(NA, KB)
    main = blk[:, MAIN].ravel()
    pad = np.zeros((N, H - main.size), np.float32)
    t5m = np.concatenate([cr[:, main], pad, ci[:, main], pad], 1)

    def stack(part):
        idx = blk[:, TAIL[list(part)]].ravel()
        t = _np_split(np.concatenate([cr[:, idx], ci[:, idx]], 1))
        return np.concatenate([t[i] for i, _ in PAIRS], 1)

    return cs, _np_split(t1), _np_split(t5m), stack(MIDS), stack(ENDS)


def _split(x):
    h = x.astype(BF16)
    r = x - h.astype(F32)
    m = r.astype(BF16)
    return h, m, (r - m.astype(F32)).astype(BF16)


PAIRS = ((0, 0), (1, 0), (2, 0), (0, 1), (1, 1), (0, 2))


def _dot6(ls, rs):
    acc = None
    for i, j in PAIRS:
        d = jnp.dot(ls[i], rs[j], preferred_element_type=F32)
        acc = d if acc is None else acc + d
    return acc


def _late_part(v_ref, part, yr, tab):
    def half(lanes):
        return [v_ref[n * NTP + t:n * NTP + t + 1, yr, lanes] for n in range(NA) for t in part]

    t = jnp.swapaxes(jnp.concatenate(half(slice(0, H)) + half(slice(H, N)), axis=0), 0, 1)
    outs = []
    for q in range(G // 2):
        p = _split(jnp.concatenate([t[2 * q], t[2 * q + 1]], axis=1))
        p = [x.astype(F32) for x in p]
        x = jnp.concatenate([p[k] for _, k in PAIRS], axis=0).astype(BF16)
        acc = jnp.dot(tab, x, preferred_element_type=F32)
        outs += [acc[:, :H], acc[:, H:]]
    return jnp.swapaxes(jnp.stack(outs), 0, 1)


def _k2(t_ref, w_ref, v_ref, o_ref, buf, osem):
    def yr(j):
        return pl.ds(pl.multiple_of(j * G, G), G)

    def wr(j):
        return pltpu.make_async_copy(buf.at[j], o_ref.at[:, yr(j), :], osem.at[j])

    @pl.loop(0, NG)
    def _(j):
        buf[j] = w_ref[j] + _late_part(v_ref, ENDS, yr(j), t_ref[...])
        wr(j).start()

    @pl.loop(0, NG)
    def _(j):
        wr(j).wait()


def _k1(t1_ref, t5_hbm, t6_hbm, cs_hbm, u_ref, g_ref, w_ref, vt_ref, t5_ref, t6_ref, cs_ref, gx,
        us, v4, xs, r1, y2, r2, r3, gv, w3, w3i, t4,
        gp, za, zs, ya, fa, zb, vx,
        usem, gsem, s1, q1, s2, q2, s3, q3, s4, q4,
        gpsem, sg, qg, sa1, qa1, sa3, qa3, sa6, qa6, sa8, qa8, q4t,
        tsem, sgx, qgx):
    a = lax.axis_index("a")
    b = lax.axis_index("b")
    ob = 1 - b

    def ucopy(j):
        return pltpu.make_async_copy(
            u_ref.at[:, pl.ds(pl.multiple_of(j * G, G), G), :], us.at[lax.rem(j, US)],
            usem.at[lax.rem(j, US)])

    def gcopy(k):
        return pltpu.make_async_copy(g_ref.at[k], gv.at[lax.rem(k, GS)], gsem.at[lax.rem(k, GS)])

    nk = KB - lax.rem(a, 2) * (1 + a // 3)

    @pl.loop(0, US)
    def _(j):
        ucopy(j).start()

    cscopy = pltpu.make_async_copy(cs_hbm, cs_ref, tsem.at[0])
    t5copy = pltpu.make_async_copy(t5_hbm, t5_ref, tsem.at[1])
    t6copy = pltpu.make_async_copy(t6_hbm, t6_ref, tsem.at[2])
    cscopy.start()
    t5copy.start()
    t6copy.start()
    for n in (2 * NTP - 1, 4 * NTP - 2, 4 * NTP - 1):
        vt_ref[n] = jnp.zeros((YA, N), F32)

    barrier = pltpu.get_barrier_semaphore()
    for d in range(1, NA):
        pl.semaphore_signal(barrier, inc=1, device_id=(b, lax.rem(a + d, NA)), device_id_type=MESH)
    pl.semaphore_signal(barrier, inc=1, device_id=(ob, a), device_id_type=MESH)

    def rows(blk):
        return pl.ds(pl.multiple_of(blk * YA, YA), YA)

    own = pl.ds(pl.multiple_of(b * H, H), H)
    oth = pl.ds(pl.multiple_of(ob * H, H), H)

    def cls(k):
        return jnp.maximum(k - (REG - 1), 0)

    def used(blk, k):
        return lax.rem(blk, 2) * (1 + blk // 3) < KB - k

    own_first, own_last = own, oth

    def home(blk, k):
        if isinstance(k, int) and k == REG - 1:
            return blk * KB + k - (blk // 3) * (2 * KB - 2)
        return blk * KB + k

    def e1(k, to, sem=0):
        return pltpu.make_async_remote_copy(
            src_ref=xs.at[home(to, k)],
            dst_ref=r1.at[k - ALT, rows(a)],
            send_sem=s1.at[sem], recv_sem=q1.at[k], device_id=(b, to), device_id_type=MESH)

    def e1_group(k, j, to):
        return pltpu.make_async_remote_copy(
            src_ref=xs.at[to * KB + k, pl.ds(pl.multiple_of(j * G, G), G)],
            dst_ref=r1.at[k - ALT, pl.ds(pl.multiple_of(a * YA + j * G, G), G)],
            send_sem=s1.at[0], recv_sem=q1.at[k], device_id=(b, to), device_id_type=MESH)

    def e2(k):
        return pltpu.make_async_remote_copy(
            src_ref=y2.at[k - ALT, oth], dst_ref=r2.at[k - ALT],
            send_sem=s2.at[cls(k)], recv_sem=q2.at[lax.rem(k, QS)], device_id=(ob, a), device_id_type=MESH)

    def e3(k):
        return pltpu.make_async_remote_copy(
            src_ref=r2.at[k - ALT], dst_ref=r3.at[k - ALT],
            send_sem=s3.at[cls(k)], recv_sem=q3.at[lax.rem(k, QS)], device_id=(ob, a), device_id_type=MESH)

    def e4(k, to):
        return pltpu.make_async_remote_copy(
            src_ref=r1.at[k - ALT, rows(to)], dst_ref=v4.at[a * NM + k - ALT],
            send_sem=s4.at[0], recv_sem=q4, device_id=(b, to), device_id_type=MESH)

    def e4_tail(k, n, to):
        return pltpu.make_async_remote_copy(
            src_ref=r1.at[k - ALT, rows(to)], dst_ref=vt_ref.at[a * NTP + k - NM],
            send_sem=s4.at[cls(k)], recv_sem=q4t.at[cls(k) * 3 + n], device_id=(b, to), device_id_type=MESH)

    gp_own = pltpu.make_async_copy(g_ref.at[b], gp.at[pl.ds(0, H)], gpsem)

    def gp_other():
        return pltpu.make_async_remote_copy(
            src_ref=g_ref.at[ob], dst_ref=gp.at[pl.ds(H, H)],
            send_sem=sg, recv_sem=qg, device_id=(ob, a), device_id_type=MESH)

    def a1(n, j):
        yr = pl.ds(pl.multiple_of(j * G, G), G)
        return pltpu.make_async_remote_copy(
            src_ref=xs.at[n * KB + ob, yr], dst_ref=za.at[n, yr],
            send_sem=sa1, recv_sem=qa1, device_id=(ob, a), device_id_type=MESH)

    def a3(to):
        return pltpu.make_async_remote_copy(
            src_ref=zs.at[to], dst_ref=ya.at[rows(a)],
            send_sem=sa3, recv_sem=qa3, device_id=(b, to), device_id_type=MESH)

    def a6(to):
        return pltpu.make_async_remote_copy(
            src_ref=ya.at[rows(to)], dst_ref=zb.at[a],
            send_sem=sa6, recv_sem=qa6, device_id=(b, to), device_id_type=MESH)

    def a8(n):
        return pltpu.make_async_remote_copy(
            src_ref=vx.at[n], dst_ref=vt_ref.at[n * NTP + b],
            send_sem=sa8, recv_sem=qa8, device_id=(ob, a), device_id_type=MESH)

    def wait_bytes(ref, sem):
        pltpu.make_async_copy(ref, ref, sem).wait()

    others = [lax.rem(a + d, NA) for d in (2, 1, 3)]
    senders = [lax.rem(a + NA - d, NA) for d in (2, 1, 3)]

    gxcopy = pltpu.make_async_remote_copy(
        src_ref=g_ref.at[KB - 1], dst_ref=gx, send_sem=sgx, recv_sem=qgx,
        device_id=(b, 3), device_id_type=MESH)

    @pl.loop(0, NG)
    def _(j):
        ucopy(j).wait()
        t = jnp.swapaxes(us[lax.rem(j, US)], 0, 1)
        tab = [t1_ref[p] for p in range(3)]
        res, ims = [], []
        for q in range(G // 2):
            x = jnp.concatenate([t[2 * q], t[2 * q + 1]], axis=1)
            acc = _dot6(tab, _split(x))
            res += [acc[:H, :H], acc[:H, H:]]
            ims += [acc[H:, :H], acc[H:, H:]]
        re = jnp.swapaxes(jnp.stack(res), 0, 1)
        im = jnp.swapaxes(jnp.stack(ims), 0, 1)
        z = jnp.zeros((1, G, H), F32)
        yr = pl.ds(pl.multiple_of(j * G, G), G)
        xs[:H, yr, :H] = re
        xs[0:1, yr, H:] = z
        xs[1:H, yr, H:] = im[1:]
        xs[H:H + 1, yr, :H] = im[0:1]
        xs[H:H + 1, yr, H:] = z
        xs[H + 1:, yr, :] = jnp.zeros((NA * KB - H - 1, G, N), F32)
        r1[:, pl.ds(pl.multiple_of(a * YA + j * G, G), G), :] = xs[pl.ds(a * KB + ALT, NP), yr, :]
        r1[REG - 1 - ALT, pl.ds(pl.multiple_of(a * YA + j * G, G), G), :] = xs[home(a, REG - 1), yr, :]

        @pl.when(j + US < NG)
        def _():
            ucopy(j + US).start()

        @pl.when(j == 0)
        def _():
            pl.semaphore_wait(barrier, NA)
            gp_other().start()

            @pl.when(a == 1)
            def _():
                gxcopy.start()

        for k in range(ALT, ALT + EARLY):
            for to in others:
                e1_group(k, j, to).start()
        for n in range(NA):
            a1(n, j).start()

    @pl.loop(ALT + EARLY, REG - 1)
    def _(k):
        for to in others:
            e1(k, to).start()

    for to in others:
        e1(REG - 1, to).start()
    for k in (REG, REG + 1):
        for n, to in enumerate(others):
            @pl.when(used(to, k))
            def _():
                e1(k, to, 1 + (k - REG) * 3 + n).start()

    cscopy.wait()

    @pl.loop(ALT, ALT + GS)
    def _(k):
        gcopy(k).start()

    gp_own.start()

    def tables():
        for p in range(3):
            for k, sl in ((0, own), (1, oth)):
                cr, sr = cs_ref[p, 0, sl, :], cs_ref[p, 1, sl, :]
                w3[p, k * N:k * N + H, :N] = cr
                w3[p, k * N:k * N + H, N:] = -sr
                w3[p, k * N + H:(k + 1) * N, :N] = sr
                w3[p, k * N + H:(k + 1) * N, N:] = cr
                cc = (cs_ref[p, 0, :, sl].astype(F32) * (1.0 / N)).astype(BF16)
                sc = (cs_ref[p, 1, :, sl].astype(F32) * (1.0 / N)).astype(BF16)
                w3i[p, :N, k * N:k * N + H] = cc
                w3i[p, :N, k * N + H:(k + 1) * N] = sc
                w3i[p, N:, k * N:k * N + H] = -sc
                w3i[p, N:, k * N + H:(k + 1) * N] = cc
                t4[p, :N, k * H:(k + 1) * H] = cc
                t4[p, N:, k * H:(k + 1) * H] = sc

    def stage2(k):
        wait_bytes(r1.at[k - ALT, pl.ds(0, (NA - 1) * YA)], q1.at[k])
        acc = _dot6([cs_ref[q].reshape(2 * N, N) for q in range(3)], _split(r1[k - ALT]))
        y2[k - ALT, :, :H] = acc[:N, :H] + acc[N:, H:]
        y2[k - ALT, :, H:] = acc[:N, H:] - acc[N:, :H]
        e2(k).start()

    def stage3(k):
        e2(k).wait_recv()
        x = _split(jnp.concatenate([y2[k - ALT, own, :], r2[k - ALT]], axis=1))
        z = _dot6(x, [w3[q] for q in range(3)])
        gcopy(k).wait()

        @pl.when(jnp.logical_and(k == REG - 1, a == 3))
        def _():
            gxcopy.wait_recv()
            gv[(REG - 1) % GS] = gx[...]

        gk = gv[lax.rem(k, GS)]
        z = _split(jnp.concatenate([z[:, :N] * gk, z[:, N:] * gk], axis=1))
        z = _dot6(z, [w3i[q] for q in range(3)])
        y2[k - ALT, own, :] = z[:, :N]
        r2[k - ALT] = z[:, N:]
        e3(k).start()

        @pl.when(k + GS < nk)
        def _():
            gcopy(k + GS).start()

    def stage4(k):
        e3(k).wait_recv()
        x = jnp.concatenate([y2[k - ALT, own, :], r3[k - ALT]], axis=0)
        acc = _dot6([t4[q] for q in range(3)], _split(x))
        r1[k - ALT, :, :H] = acc[:N, :H] - acc[N:, H:]
        r1[k - ALT, :, H:] = acc[:N, H:] + acc[N:, :H]

        @pl.when(k < ALT + NM)
        def _():
            for to in others:
                e4(k, to).start()
            v4[a * NM + k - ALT] = r1[k - ALT, rows(a), :]

        @pl.when(k >= ALT + NM)
        def _():
            for n, to in enumerate(others):
                e4_tail(k, n, to).start()
            vt_ref[a * NTP + k - NM] = r1[k - ALT, rows(a), :]

    def alt_z():
        wait_bytes(za, qa1)
        x = jnp.concatenate([xs[n * KB + b] for n in range(NA)], axis=0)
        x = jnp.concatenate([x, za[...].reshape(NA * YA, N)], axis=1)
        zs[...] = _dot6(_split(x), [w3[q] for q in range(3)]).reshape(NA, YA, 2 * N)
        for to in others:
            a3(to).start()
        ya[rows(a), :] = zs[a]

    def alt_y():
        wait_bytes(zs.at[pl.ds(0, NA - 1)], qa3)
        wait_bytes(gp.at[pl.ds(H, H)], qg)
        gp_own.wait()
        for q in range(2):
            x = jnp.concatenate([ya[:, q * H:(q + 1) * H], ya[:, N + q * H:N + (q + 1) * H]], axis=1)
            acc = _dot6([cs_ref[p].reshape(2 * N, N) for p in range(3)], _split(x))
            re = acc[:N, :H] + acc[N:, H:]
            im = acc[:N, H:] - acc[N:, :H]
            fa[own_first, :H], fa[own_first, H:] = re[:H], im[:H]
            fa[own_last, :H], fa[own_last, H:] = re[H:], im[H:]
            gq = gp[:, q * H:(q + 1) * H]
            x = fa[...] * jnp.concatenate([gq, gq], axis=1)
            acc = _dot6([t4[p] for p in range(3)], _split(x))
            ya[:, q * H:(q + 1) * H] = acc[:N, :H] - acc[N:, H:]
            ya[:, N + q * H:N + (q + 1) * H] = acc[:N, H:] + acc[N:, :H]
        for to in others:
            a6(to).start()
        zb[a] = ya[rows(a), :]

    def alt_zinv():
        wait_bytes(zs.at[pl.ds(0, NA - 1)], qa6)
        z = _dot6(_split(zb[...].reshape(NA * YA, 2 * N)), [w3i[q] for q in range(3)])
        vx[...] = z[:, N:].reshape(NA, YA, N)
        for n in range(NA):
            vt_ref[n * NTP + b] = z[n * YA:(n + 1) * YA, :N]

    def inv_x(j):
        yr = pl.ds(pl.multiple_of(j * G, G), G)
        z = jnp.zeros((H - NA * NM, G, H), F32)
        re = jnp.swapaxes(jnp.concatenate([v4[:, yr, :H], z], axis=0), 0, 1)
        im = jnp.swapaxes(jnp.concatenate([v4[:, yr, H:], z], axis=0), 0, 1)
        tab = [t5_ref[p] for p in range(3)]
        outs = []
        for q in range(G // 2):
            x = jnp.concatenate([
                jnp.concatenate([re[2 * q], re[2 * q + 1]], axis=1),
                jnp.concatenate([im[2 * q], im[2 * q + 1]], axis=1)], axis=0)
            acc = _dot6(tab, _split(x))
            outs += [acc[:, :H], acc[:, H:]]
        w_ref[j] = jnp.swapaxes(jnp.stack(outs), 0, 1)

    @pl.loop(ALT, KB + A2 + A3)
    def _(i):
        @pl.when(i < nk)
        def _():
            stage2(i)

        @pl.when(i == ALT)
        def _():
            tables()
            alt_z()

        @pl.when(jnp.logical_and(i >= ALT + A2, i < nk + A2))
        def _():
            stage3(i - A2)

        @pl.when(i == MID)
        def _():
            alt_y()

        @pl.when(i == LATE)
        def _():
            alt_zinv()

        @pl.when(i == KB + A2 - 1)
        def _():
            for n in range(NA):
                a8(n).start()

        @pl.when(jnp.logical_and(i >= ALT + A2 + A3, i < nk + A2 + A3))
        def _():
            stage4(i - A2 - A3)

        @pl.when(i == I5)
        def _():
            wait_bytes(v4.at[pl.ds(0, (NA - 1) * NM)], q4)
            t5copy.wait()

        @pl.when(i >= I5)
        def _():
            @pl.loop((i - I5) * PG, jnp.minimum((i - I5 + 1) * PG, NG))
            def _(j):
                inv_x(j)

    def blocks(n):
        return xs.at[pl.ds(0, n)]

    for n in range(NA - 1):
        wait_bytes(blocks(REG - ALT - NM), q4t.at[n])
    t6copy.wait()

    @pl.loop(0, NG)
    def _(j):
        w_ref[j] += _late_part(vt_ref, MIDS, pl.ds(pl.multiple_of(j * G, G), G), t6_ref[...])

    nr = REG - ALT
    wait_bytes(blocks((NA - 1) * nr), s1.at[0])
    wait_bytes(blocks((NA - 1) * nr), s4.at[0])
    wait_bytes(r2.at[pl.ds(0, nr)], s2.at[0])
    wait_bytes(r2.at[pl.ds(0, nr)], s3.at[0])
    for k in (REG, REG + 1):
        c = k - REG + 1

        @pl.when(used(a, k))
        def _():
            wait_bytes(blocks(NA - 1), s4.at[c])
            wait_bytes(r2.at[0], s2.at[c])
            wait_bytes(r2.at[0], s3.at[c])

        for n in range(NA - 1):
            @pl.when(used(others[n], k))
            def _():
                wait_bytes(xs.at[0], s1.at[1 + (k - REG) * 3 + n])

            @pl.when(used(senders[n], k))
            def _():
                wait_bytes(xs.at[0], q4t.at[c * 3 + n])

    @pl.when(a == 1)
    def _():
        gxcopy.wait_send()

    wait_bytes(gp.at[pl.ds(0, H)], sg)
    wait_bytes(za, sa1)
    wait_bytes(zs.at[pl.ds(0, NA - 1)], sa3)
    wait_bytes(zs.at[pl.ds(0, NA - 1)], sa6)
    wait_bytes(za, sa8)
    wait_bytes(za, qa8)


def solution(mesh):
    tables = _np_tables()
    dma = pltpu.SemaphoreType.DMA

    def local(u, g):
        cs, t1, t5m, t6, t5t = (jnp.asarray(t) for t in tables)
        any_ = pl.BlockSpec(memory_space=pl.ANY)
        vmem = pl.BlockSpec(memory_space=pltpu.VMEM)
        w, vt = pl.pallas_call(
            _k1, name="fwd_yz",
            in_specs=[vmem, any_, any_, any_, any_, any_],
            out_specs=[vmem, vmem],
            out_shape=[pltpu.VMEM((NG, N, G, H), F32), pltpu.VMEM((NT, YA, N), F32)],
            scratch_shapes=[
                pltpu.VMEM((3, N, N), BF16), pltpu.VMEM((N, 240), BF16),
                pltpu.VMEM((3, 2, N, N), BF16), pltpu.VMEM((H, N), F32),
                pltpu.VMEM((US, N, G, H), F32), pltpu.VMEM((NA * NM, YA, N), F32),
                pltpu.VMEM((NA * KB, YA, N), F32),
                pltpu.VMEM((NP, N, N), F32), pltpu.VMEM((NP, N, N), F32),
                pltpu.VMEM((NP, H, N), F32), pltpu.VMEM((NP, H, N), F32),
                pltpu.VMEM((GS, H, N), F32),
                pltpu.VMEM((3, 2 * N, 2 * N), BF16), pltpu.VMEM((3, 2 * N, 2 * N), BF16),
                pltpu.VMEM((3, 2 * N, N), BF16),
                pltpu.VMEM((N, N), F32), pltpu.VMEM((NA, YA, N), F32),
                pltpu.VMEM((NA, YA, 2 * N), F32), pltpu.VMEM((N, 2 * N), F32),
                pltpu.VMEM((N, N), F32), pltpu.VMEM((NA, YA, 2 * N), F32),
                pltpu.VMEM((NA, YA, N), F32),
                dma((US,)), dma((GS,)), dma((7,)), dma((KB,)), dma((3,)), dma((QS,)), dma((3,)), dma((QS,)),
                dma((3,)), dma,
                dma, dma, dma, dma, dma, dma, dma, dma, dma, dma, dma, dma((9,)),
                dma((3,)), dma, dma,
            ],
            compiler_params=pltpu.CompilerParams(
                collective_id=0, has_side_effects=True, vmem_limit_bytes=VM * 2**20),
        )(t1, t5m, t6, cs, u, g)
        return pl.pallas_call(
            _k2, name="inv_x",
            in_specs=[vmem, vmem, vmem], out_specs=any_,
            out_shape=jax.ShapeDtypeStruct((N, YA, H), F32),
            scratch_shapes=[
                pltpu.VMEM((NG, N, G, H), F32), dma((NG,))],
            compiler_params=pltpu.CompilerParams(vmem_limit_bytes=30 * 2**20),
        )(t5t, w, vt)

    return jax.shard_map(local, mesh=mesh, in_specs=(P(None, "a", "b"), P("a", "b", None)),
                         out_specs=P(None, "a", "b"), check_vma=False)
```

```python
import functools
import math

import jax
import jax.numpy as jnp
import numpy as np
from jax import lax
from jax.experimental import pallas as pl
from jax.experimental.pallas import tpu as pltpu
from jax.sharding import PartitionSpec as P

N = 256
H = 128
KB = 33
NA = 4
NB = 2
YA = 64
G = 8
NG = YA // G
VM = 52
US = 3
ALT = 2
EARLY = 2
MID = 20
LATE = 30
NTP = 10
NM = KB - NTP
MAIN = np.arange(ALT, ALT + NM)
MIDS = (2, 3, 4, 5, 6)
ENDS = (0, 1, 7, 8, 9)
TAIL = np.concatenate([np.arange(ALT), np.arange(ALT + NM, KB)])
NT = NA * NTP
REG = KB - 2
NP = KB - ALT
QS = 8
GS = 6
I5 = 31
PG = 3
A2 = 2
A3 = 2
F32 = jnp.float32
BF16 = jnp.bfloat16
MESH = pl.DeviceIdType.MESH


def _np_split(x):
    x = np.asarray(x, np.float32)
    out = []
    for _ in range(3):
        p = x.astype(jnp.bfloat16)
        out.append(p)
        x = x - p.astype(np.float32)
    return np.stack(out)


def _np_tables():
    r = np.arange(N)
    ang = ((r[:, None] * r[None, :]) % N).astype(np.float32) * np.float32(2.0 * math.pi / N)
    c = np.cos(ang.astype(np.float64)).astype(np.float32)
    s = np.sin(ang.astype(np.float64)).astype(np.float32)
    cs = np.stack([_np_split(c), _np_split(s)], 1)
    t1 = np.concatenate([c[:H + 1], -s[1:H]], 0)
    kx = np.arange(NA * KB)
    kx[3 * KB + REG - 1] = 2 * KB - 1
    kx[[2 * KB - 1, 4 * KB - 2, 4 * KB - 1]] = NA * KB
    wgt = np.where((kx == 0) | (kx == H), 1.0, 2.0) * (kx <= H) / N
    kc = np.minimum(kx, N - 1)
    cr = (c[:, kc] * wgt).astype(np.float32)
    ci = (-s[:, kc] * wgt).astype(np.float32)
    blk = np.arange(NA * KB).reshape(NA, KB)
    main = blk[:, MAIN].ravel()
    pad = np.zeros((N, H - main.size), np.float32)
    t5m = np.concatenate([cr[:, main], pad, ci[:, main], pad], 1)

    def stack(part):
        idx = blk[:, TAIL[list(part)]].ravel()
        t = _np_split(np.concatenate([cr[:, idx], ci[:, idx]], 1))
        return np.concatenate([t[i] for i, _ in PAIRS], 1)

    return cs, _np_split(t1), _np_split(t5m), stack(MIDS), stack(ENDS)


def _split(x):
    h = x.astype(BF16)
    r = x - h.astype(F32)
    m = r.astype(BF16)
    return h, m, (r - m.astype(F32)).astype(BF16)


PAIRS = ((0, 0), (1, 0), (2, 0), (0, 1), (1, 1), (0, 2))


def _dot6(ls, rs):
    acc = None
    for i, j in PAIRS:
        d = jnp.dot(ls[i], rs[j], preferred_element_type=F32)
        acc = d if acc is None else acc + d
    return acc


def _late_part(v_ref, part, yr, tab):
    def half(lanes):
        return [v_ref[n * NTP + t:n * NTP + t + 1, yr, lanes] for n in range(NA) for t in part]

    t = jnp.swapaxes(jnp.concatenate(half(slice(0, H)) + half(slice(H, N)), axis=0), 0, 1)
    outs = []
    for q in range(G // 2):
        p = _split(jnp.concatenate([t[2 * q], t[2 * q + 1]], axis=1))
        p = [x.astype(F32) for x in p]
        x = jnp.concatenate([p[k] for _, k in PAIRS], axis=0).astype(BF16)
        acc = jnp.dot(tab, x, preferred_element_type=F32)
        outs += [acc[:, :H], acc[:, H:]]
    return jnp.swapaxes(jnp.stack(outs), 0, 1)


def _k2(t_ref, w_ref, v_ref, o_ref, buf, osem):
    def yr(j):
        return pl.ds(pl.multiple_of(j * G, G), G)

    def wr(j):
        return pltpu.make_async_copy(buf.at[j], o_ref.at[:, yr(j), :], osem.at[j])

    @pl.loop(0, NG)
    def _(j):
        buf[j] = w_ref[j] + _late_part(v_ref, ENDS, yr(j), t_ref[...])
        wr(j).start()

    @pl.loop(0, NG)
    def _(j):
        wr(j).wait()


def _k1(t1_hbm, t5_hbm, t6_hbm, cs_hbm, u_ref, g_ref, w_ref, vt_ref, t1_ref, t5_ref, t6_ref,
        cs_ref, gx, us, v4, xs, r1, y2, r2, r3, gv, w3, w3i, t4,
        gp, za, zs, ya, fa, zb, vx,
        usem, gsem, s1, q1, s2, q2, s3, q3, s4, q4,
        gpsem, sg, qg, sa1, qa1, sa3, qa3, sa6, qa6, sa8, qa8, q4t,
        tsem, sgx, qgx):
    a = lax.axis_index("a")
    b = lax.axis_index("b")
    ob = 1 - b

    def ucopy(j):
        return pltpu.make_async_copy(
            u_ref.at[:, pl.ds(pl.multiple_of(j * G, G), G), :], us.at[lax.rem(j, US)],
            usem.at[lax.rem(j, US)])

    def gcopy(k):
        return pltpu.make_async_copy(g_ref.at[k], gv.at[lax.rem(k, GS)], gsem.at[lax.rem(k, GS)])

    nk = KB - lax.rem(a, 2) * (1 + a // 3)

    ucopy(0).start()
    t1copy = pltpu.make_async_copy(t1_hbm, t1_ref, tsem.at[3])
    t1copy.start()

    @pl.loop(1, US)
    def _(j):
        ucopy(j).start()

    cscopy = pltpu.make_async_copy(cs_hbm, cs_ref, tsem.at[0])
    t5copy = pltpu.make_async_copy(t5_hbm, t5_ref, tsem.at[1])
    t6copy = pltpu.make_async_copy(t6_hbm, t6_ref, tsem.at[2])
    cscopy.start()
    t5copy.start()
    t6copy.start()
    for n in (2 * NTP - 1, 4 * NTP - 2, 4 * NTP - 1):
        vt_ref[n] = jnp.zeros((YA, N), F32)

    barrier = pltpu.get_barrier_semaphore()
    for d in range(1, NA):
        pl.semaphore_signal(barrier, inc=1, device_id=(b, lax.rem(a + d, NA)), device_id_type=MESH)
    pl.semaphore_signal(barrier, inc=1, device_id=(ob, a), device_id_type=MESH)

    def rows(blk):
        return pl.ds(pl.multiple_of(blk * YA, YA), YA)

    own = pl.ds(pl.multiple_of(b * H, H), H)
    oth = pl.ds(pl.multiple_of(ob * H, H), H)

    def cls(k):
        return jnp.maximum(k - (REG - 1), 0)

    def used(blk, k):
        return lax.rem(blk, 2) * (1 + blk // 3) < KB - k

    own_first, own_last = own, oth

    def home(blk, k):
        if isinstance(k, int) and k == REG - 1:
            return blk * KB + k - (blk // 3) * (2 * KB - 2)
        return blk * KB + k

    def e1(k, to, sem=0):
        return pltpu.make_async_remote_copy(
            src_ref=xs.at[home(to, k)],
            dst_ref=r1.at[k - ALT, rows(a)],
            send_sem=s1.at[sem], recv_sem=q1.at[k], device_id=(b, to), device_id_type=MESH)

    def e1_group(k, j, to):
        return pltpu.make_async_remote_copy(
            src_ref=xs.at[to * KB + k, pl.ds(pl.multiple_of(j * G, G), G)],
            dst_ref=r1.at[k - ALT, pl.ds(pl.multiple_of(a * YA + j * G, G), G)],
            send_sem=s1.at[0], recv_sem=q1.at[k], device_id=(b, to), device_id_type=MESH)

    def e2(k):
        return pltpu.make_async_remote_copy(
            src_ref=y2.at[k - ALT, oth], dst_ref=r2.at[k - ALT],
            send_sem=s2.at[cls(k)], recv_sem=q2.at[lax.rem(k, QS)], device_id=(ob, a), device_id_type=MESH)

    def e3(k):
        return pltpu.make_async_remote_copy(
            src_ref=r2.at[k - ALT], dst_ref=r3.at[k - ALT],
            send_sem=s3.at[cls(k)], recv_sem=q3.at[lax.rem(k, QS)], device_id=(ob, a), device_id_type=MESH)

    def e4(k, to):
        return pltpu.make_async_remote_copy(
            src_ref=r1.at[k - ALT, rows(to)], dst_ref=v4.at[a * NM + k - ALT],
            send_sem=s4.at[0], recv_sem=q4, device_id=(b, to), device_id_type=MESH)

    def e4_tail(k, n, to):
        return pltpu.make_async_remote_copy(
            src_ref=r1.at[k - ALT, rows(to)], dst_ref=vt_ref.at[a * NTP + k - NM],
            send_sem=s4.at[cls(k)], recv_sem=q4t.at[cls(k) * 3 + n], device_id=(b, to), device_id_type=MESH)

    gp_own = pltpu.make_async_copy(g_ref.at[b], gp.at[pl.ds(0, H)], gpsem)

    def gp_other():
        return pltpu.make_async_remote_copy(
            src_ref=g_ref.at[ob], dst_ref=gp.at[pl.ds(H, H)],
            send_sem=sg, recv_sem=qg, device_id=(ob, a), device_id_type=MESH)

    def a1(n, j):
        yr = pl.ds(pl.multiple_of(j * G, G), G)
        return pltpu.make_async_remote_copy(
            src_ref=xs.at[n * KB + ob, yr], dst_ref=za.at[n, yr],
            send_sem=sa1, recv_sem=qa1, device_id=(ob, a), device_id_type=MESH)

    def a3(to):
        return pltpu.make_async_remote_copy(
            src_ref=zs.at[to], dst_ref=ya.at[rows(a)],
            send_sem=sa3, recv_sem=qa3, device_id=(b, to), device_id_type=MESH)

    def a6(to):
        return pltpu.make_async_remote_copy(
            src_ref=ya.at[rows(to)], dst_ref=zb.at[a],
            send_sem=sa6, recv_sem=qa6, device_id=(b, to), device_id_type=MESH)

    def a8(n):
        return pltpu.make_async_remote_copy(
            src_ref=vx.at[n], dst_ref=vt_ref.at[n * NTP + b],
            send_sem=sa8, recv_sem=qa8, device_id=(ob, a), device_id_type=MESH)

    def wait_bytes(ref, sem):
        pltpu.make_async_copy(ref, ref, sem).wait()

    others = [lax.rem(a + d, NA) for d in (2, 1, 3)]
    senders = [lax.rem(a + NA - d, NA) for d in (2, 1, 3)]

    gxcopy = pltpu.make_async_remote_copy(
        src_ref=g_ref.at[KB - 1], dst_ref=gx, send_sem=sgx, recv_sem=qgx,
        device_id=(b, 3), device_id_type=MESH)

    t1copy.wait()

    @pl.loop(0, NG)
    def _(j):
        ucopy(j).wait()
        t = jnp.swapaxes(us[lax.rem(j, US)], 0, 1)
        tab = [t1_ref[p] for p in range(3)]
        res, ims = [], []
        for q in range(G // 2):
            x = jnp.concatenate([t[2 * q], t[2 * q + 1]], axis=1)
            acc = _dot6(tab, _split(x))
            res += [acc[:H, :H], acc[:H, H:]]
            ims += [acc[H:, :H], acc[H:, H:]]
        re = jnp.swapaxes(jnp.stack(res), 0, 1)
        im = jnp.swapaxes(jnp.stack(ims), 0, 1)
        z = jnp.zeros((1, G, H), F32)
        yr = pl.ds(pl.multiple_of(j * G, G), G)
        xs[:H, yr, :H] = re
        xs[0:1, yr, H:] = z
        xs[1:H, yr, H:] = im[1:]
        xs[H:H + 1, yr, :H] = im[0:1]
        xs[H:H + 1, yr, H:] = z
        xs[H + 1:, yr, :] = jnp.zeros((NA * KB - H - 1, G, N), F32)
        r1[:, pl.ds(pl.multiple_of(a * YA + j * G, G), G), :] = xs[pl.ds(a * KB + ALT, NP), yr, :]
        r1[REG - 1 - ALT, pl.ds(pl.multiple_of(a * YA + j * G, G), G), :] = xs[home(a, REG - 1), yr, :]

        @pl.when(j + US < NG)
        def _():
            ucopy(j + US).start()

        @pl.when(j == 0)
        def _():
            pl.semaphore_wait(barrier, NA)
            gp_other().start()

            @pl.when(a == 1)
            def _():
                gxcopy.start()

        for k in range(ALT, ALT + EARLY):
            for to in others:
                e1_group(k, j, to).start()
        for n in range(NA):
            a1(n, j).start()

    @pl.loop(ALT + EARLY, REG - 1)
    def _(k):
        for to in others:
            e1(k, to).start()

    for to in others:
        e1(REG - 1, to).start()
    for k in (REG, REG + 1):
        for n, to in enumerate(others):
            @pl.when(used(to, k))
            def _():
                e1(k, to, 1 + (k - REG) * 3 + n).start()

    cscopy.wait()

    @pl.loop(ALT, ALT + GS)
    def _(k):
        gcopy(k).start()

    gp_own.start()

    def tables():
        for p in range(3):
            for k, sl in ((0, own), (1, oth)):
                cr, sr = cs_ref[p, 0, sl, :], cs_ref[p, 1, sl, :]
                w3[p, k * N:k * N + H, :N] = cr
                w3[p, k * N:k * N + H, N:] = -sr
                w3[p, k * N + H:(k + 1) * N, :N] = sr
                w3[p, k * N + H:(k + 1) * N, N:] = cr
                cc = (cs_ref[p, 0, :, sl].astype(F32) * (1.0 / N)).astype(BF16)
                sc = (cs_ref[p, 1, :, sl].astype(F32) * (1.0 / N)).astype(BF16)
                w3i[p, :N, k * N:k * N + H] = cc
                w3i[p, :N, k * N + H:(k + 1) * N] = sc
                w3i[p, N:, k * N:k * N + H] = -sc
                w3i[p, N:, k * N + H:(k + 1) * N] = cc
                t4[p, :N, k * H:(k + 1) * H] = cc
                t4[p, N:, k * H:(k + 1) * H] = sc

    def stage2(k):
        wait_bytes(r1.at[k - ALT, pl.ds(0, (NA - 1) * YA)], q1.at[k])
        acc = _dot6([cs_ref[q].reshape(2 * N, N) for q in range(3)], _split(r1[k - ALT]))
        y2[k - ALT, :, :H] = acc[:N, :H] + acc[N:, H:]
        y2[k - ALT, :, H:] = acc[:N, H:] - acc[N:, :H]
        e2(k).start()

    def stage3(k):
        e2(k).wait_recv()
        x = _split(jnp.concatenate([y2[k - ALT, own, :], r2[k - ALT]], axis=1))
        z = _dot6(x, [w3[q] for q in range(3)])
        gcopy(k).wait()

        @pl.when(jnp.logical_and(k == REG - 1, a == 3))
        def _():
            gxcopy.wait_recv()
            gv[(REG - 1) % GS] = gx[...]

        gk = gv[lax.rem(k, GS)]
        z = _split(jnp.concatenate([z[:, :N] * gk, z[:, N:] * gk], axis=1))
        z = _dot6(z, [w3i[q] for q in range(3)])
        y2[k - ALT, own, :] = z[:, :N]
        r2[k - ALT] = z[:, N:]
        e3(k).start()

        @pl.when(k + GS < nk)
        def _():
            gcopy(k + GS).start()

    def stage4(k):
        e3(k).wait_recv()
        x = jnp.concatenate([y2[k - ALT, own, :], r3[k - ALT]], axis=0)
        acc = _dot6([t4[q] for q in range(3)], _split(x))
        r1[k - ALT, :, :H] = acc[:N, :H] - acc[N:, H:]
        r1[k - ALT, :, H:] = acc[:N, H:] + acc[N:, :H]

        @pl.when(k < ALT + NM)
        def _():
            for to in others:
                e4(k, to).start()
            v4[a * NM + k - ALT] = r1[k - ALT, rows(a), :]

        @pl.when(k >= ALT + NM)
        def _():
            for n, to in enumerate(others):
                e4_tail(k, n, to).start()
            vt_ref[a * NTP + k - NM] = r1[k - ALT, rows(a), :]

    def alt_z():
        wait_bytes(za, qa1)
        x = jnp.concatenate([xs[n * KB + b] for n in range(NA)], axis=0)
        x = jnp.concatenate([x, za[...].reshape(NA * YA, N)], axis=1)
        zs[...] = _dot6(_split(x), [w3[q] for q in range(3)]).reshape(NA, YA, 2 * N)
        for to in others:
            a3(to).start()
        ya[rows(a), :] = zs[a]

    def alt_y():
        wait_bytes(zs.at[pl.ds(0, NA - 1)], qa3)
        wait_bytes(gp.at[pl.ds(H, H)], qg)
        gp_own.wait()
        for q in range(2):
            x = jnp.concatenate([ya[:, q * H:(q + 1) * H], ya[:, N + q * H:N + (q + 1) * H]], axis=1)
            acc = _dot6([cs_ref[p].reshape(2 * N, N) for p in range(3)], _split(x))
            re = acc[:N, :H] + acc[N:, H:]
            im = acc[:N, H:] - acc[N:, :H]
            fa[own_first, :H], fa[own_first, H:] = re[:H], im[:H]
            fa[own_last, :H], fa[own_last, H:] = re[H:], im[H:]
            gq = gp[:, q * H:(q + 1) * H]
            x = fa[...] * jnp.concatenate([gq, gq], axis=1)
            acc = _dot6([t4[p] for p in range(3)], _split(x))
            ya[:, q * H:(q + 1) * H] = acc[:N, :H] - acc[N:, H:]
            ya[:, N + q * H:N + (q + 1) * H] = acc[:N, H:] + acc[N:, :H]
        for to in others:
            a6(to).start()
        zb[a] = ya[rows(a), :]

    def alt_zinv():
        wait_bytes(zs.at[pl.ds(0, NA - 1)], qa6)
        z = _dot6(_split(zb[...].reshape(NA * YA, 2 * N)), [w3i[q] for q in range(3)])
        vx[...] = z[:, N:].reshape(NA, YA, N)
        for n in range(NA):
            vt_ref[n * NTP + b] = z[n * YA:(n + 1) * YA, :N]

    def inv_x(j):
        yr = pl.ds(pl.multiple_of(j * G, G), G)
        z = jnp.zeros((H - NA * NM, G, H), F32)
        re = jnp.swapaxes(jnp.concatenate([v4[:, yr, :H], z], axis=0), 0, 1)
        im = jnp.swapaxes(jnp.concatenate([v4[:, yr, H:], z], axis=0), 0, 1)
        tab = [t5_ref[p] for p in range(3)]
        outs = []
        for q in range(G // 2):
            x = jnp.concatenate([
                jnp.concatenate([re[2 * q], re[2 * q + 1]], axis=1),
                jnp.concatenate([im[2 * q], im[2 * q + 1]], axis=1)], axis=0)
            acc = _dot6(tab, _split(x))
            outs += [acc[:, :H], acc[:, H:]]
        w_ref[j] = jnp.swapaxes(jnp.stack(outs), 0, 1)

    @pl.loop(ALT, KB + A2 + A3)
    def _(i):
        @pl.when(i < nk)
        def _():
            stage2(i)

        @pl.when(i == ALT)
        def _():
            tables()
            alt_z()

        @pl.when(jnp.logical_and(i >= ALT + A2, i < nk + A2))
        def _():
            stage3(i - A2)

        @pl.when(i == MID)
        def _():
            alt_y()

        @pl.when(i == LATE)
        def _():
            alt_zinv()

        @pl.when(i == KB + A2 - 1)
        def _():
            for n in range(NA):
                a8(n).start()

        @pl.when(jnp.logical_and(i >= ALT + A2 + A3, i < nk + A2 + A3))
        def _():
            stage4(i - A2 - A3)

        @pl.when(i == I5)
        def _():
            wait_bytes(v4.at[pl.ds(0, (NA - 1) * NM)], q4)
            t5copy.wait()

        @pl.when(i >= I5)
        def _():
            @pl.loop((i - I5) * PG, jnp.minimum((i - I5 + 1) * PG, NG))
            def _(j):
                inv_x(j)

    def blocks(n):
        return xs.at[pl.ds(0, n)]

    for n in range(NA - 1):
        wait_bytes(blocks(REG - ALT - NM), q4t.at[n])
    t6copy.wait()

    @pl.loop(0, NG)
    def _(j):
        w_ref[j] += _late_part(vt_ref, MIDS, pl.ds(pl.multiple_of(j * G, G), G), t6_ref[...])

    nr = REG - ALT
    wait_bytes(blocks((NA - 1) * nr), s1.at[0])
    wait_bytes(blocks((NA - 1) * nr), s4.at[0])
    wait_bytes(r2.at[pl.ds(0, nr)], s2.at[0])
    wait_bytes(r2.at[pl.ds(0, nr)], s3.at[0])
    for k in (REG, REG + 1):
        c = k - REG + 1

        @pl.when(used(a, k))
        def _():
            wait_bytes(blocks(NA - 1), s4.at[c])
            wait_bytes(r2.at[0], s2.at[c])
            wait_bytes(r2.at[0], s3.at[c])

        for n in range(NA - 1):
            @pl.when(used(others[n], k))
            def _():
                wait_bytes(xs.at[0], s1.at[1 + (k - REG) * 3 + n])

            @pl.when(used(senders[n], k))
            def _():
                wait_bytes(xs.at[0], q4t.at[c * 3 + n])

    @pl.when(a == 1)
    def _():
        gxcopy.wait_send()

    wait_bytes(gp.at[pl.ds(0, H)], sg)
    wait_bytes(za, sa1)
    wait_bytes(zs.at[pl.ds(0, NA - 1)], sa3)
    wait_bytes(zs.at[pl.ds(0, NA - 1)], sa6)
    wait_bytes(za, sa8)
    wait_bytes(za, qa8)


def solution(mesh):
    tables = _np_tables()
    dma = pltpu.SemaphoreType.DMA

    def local(u, g):
        cs, t1, t5m, t6, t5t = (jnp.asarray(t) for t in tables)
        any_ = pl.BlockSpec(memory_space=pl.ANY)
        vmem = pl.BlockSpec(memory_space=pltpu.VMEM)
        w, vt = pl.pallas_call(
            _k1, name="fwd_yz",
            in_specs=[any_] * 6,
            out_specs=[vmem, vmem],
            out_shape=[pltpu.VMEM((NG, N, G, H), F32), pltpu.VMEM((NT, YA, N), F32)],
            scratch_shapes=[
                pltpu.VMEM((3, N, N), BF16), pltpu.VMEM((3, N, N), BF16), pltpu.VMEM((N, 240), BF16),
                pltpu.VMEM((3, 2, N, N), BF16), pltpu.VMEM((H, N), F32),
                pltpu.VMEM((US, N, G, H), F32), pltpu.VMEM((NA * NM, YA, N), F32),
                pltpu.VMEM((NA * KB, YA, N), F32),
                pltpu.VMEM((NP, N, N), F32), pltpu.VMEM((NP, N, N), F32),
                pltpu.VMEM((NP, H, N), F32), pltpu.VMEM((NP, H, N), F32),
                pltpu.VMEM((GS, H, N), F32),
                pltpu.VMEM((3, 2 * N, 2 * N), BF16), pltpu.VMEM((3, 2 * N, 2 * N), BF16),
                pltpu.VMEM((3, 2 * N, N), BF16),
                pltpu.VMEM((N, N), F32), pltpu.VMEM((NA, YA, N), F32),
                pltpu.VMEM((NA, YA, 2 * N), F32), pltpu.VMEM((N, 2 * N), F32),
                pltpu.VMEM((N, N), F32), pltpu.VMEM((NA, YA, 2 * N), F32),
                pltpu.VMEM((NA, YA, N), F32),
                dma((US,)), dma((GS,)), dma((7,)), dma((KB,)), dma((3,)), dma((QS,)), dma((3,)), dma((QS,)),
                dma((3,)), dma,
                dma, dma, dma, dma, dma, dma, dma, dma, dma, dma, dma, dma((9,)),
                dma((4,)), dma, dma,
            ],
            compiler_params=pltpu.CompilerParams(
                collective_id=0, has_side_effects=True, vmem_limit_bytes=VM * 2**20),
        )(t1, t5m, t6, cs, u, g)
        return pl.pallas_call(
            _k2, name="inv_x",
            in_specs=[vmem, vmem, vmem], out_specs=any_,
            out_shape=jax.ShapeDtypeStruct((N, YA, H), F32),
            scratch_shapes=[
                pltpu.VMEM((NG, N, G, H), F32), dma((NG,))],
            compiler_params=pltpu.CompilerParams(vmem_limit_bytes=30 * 2**20),
        )(t5t, w, vt)

    return jax.shard_map(local, mesh=mesh, in_specs=(P(None, "a", "b"), P("a", "b", None)),
                         out_specs=P(None, "a", "b"), check_vma=False)
```
